32 devices in a mesh: sec: 8 (over y, x, core), env: 4 (over z).
Axes of the slice: x: 2, y: 2, z: 4, core: 2. Of those that a mesh axis runs over, the one named last changes fastest.
Arguments:
- wavefunction: float32 [8, 512, 512], P('sec', 'env'), may hold values from -14 to 14
- left_env: bfloat16 [34, 512, 512], P(None, 'env'), may hold values from -0.176776695 to 0.176776695
- right_env: bfloat16 [34, 512, 512], P(None, 'env'), may hold values from -0.25 to 0.25
- task_in: int32 [32], replicated, may hold values from 0 to 7
- task_out: int32 [32, 1], replicated, may hold values from 0 to 7; in each aligned block of 32 rows (0 to 31, 32 to 63, ...) at most 16 rows name the same one
- task_term: int32 [32], replicated, may hold values from 0 to 33
Outputs:
- sigma: float32 [8, 512, 512], P('sec', 'env')
The draws below stay inside these ranges and needn't reach their ends.
Inputs may be any that keep to these rules, and one draw needn't show every extreme that they name: `task_out`: no sector is the target of more than 16 tasks, and in every draw some sector is the target of exactly 16.
All inputs are finite; a program needn't handle non-finite values.
Results may differ from the reference program's by a relative error of at most 0.00045.
Values may be sent and summed in bfloat16 or wider, within the bound.
No kernel may reach another device: no remote copies, remote signals or barrier semaphores. Data moves between devices by JAX's collectives and lax.ppermute only.
A program may use at most 64 MiB of HBM per device.

```python
import math
import jax
import jax.numpy as jnp
import numpy as np
from jax import lax

M = 512
TERMS = 34
CAP = 16
SECTORS = 8
TASKS = 32


def draw_wavefunction(key, part):
    offset_key, noise_key = jax.random.split(jax.random.fold_in(key, 11))
    offset = 8.0 * jax.random.uniform(offset_key, (SECTORS, 1, M), jnp.float32, -1.0, 1.0)
    noise_part = jnp.clip(jax.random.normal(noise_key, (SECTORS, M, M), jnp.float32), -4.0, 4.0)
    return (offset + noise_part).astype(jnp.float32)


def draw_left_env(key, part):
    entry_scale = 1.0 / math.sqrt(M)
    base_key = jax.random.fold_in(key, 23)
    base_draw = entry_scale * jax.random.normal(base_key, (TERMS, M, M), jnp.float32)
    centered = base_draw - 0.98 * jnp.mean(base_draw, axis=2, keepdims=True)
    return jnp.clip(centered, -4.0 * entry_scale, 4.0 * entry_scale).astype(jnp.bfloat16)


def set_ends(entries, stream_key, smallest, top_value):
    dims = entries.shape
    place = [jax.random.randint(jax.random.fold_in(stream_key, axis), (), 0, dims[axis]) for axis in range(len(dims))]
    entries = entries.at[tuple(place)].set(smallest)
    longest = dims.index(max(dims))
    place[longest] = (place[longest] + 1) % dims[longest]
    return entries.at[tuple(place)].set(top_value)


def block_scale(rng, extent, pieces, least, high):
    def one(axis_at, shards_of):
        heights = jax.random.uniform(jax.random.fold_in(jax.random.fold_in(rng, 6), axis_at), (shards_of,), jnp.float32, least / len(pieces), high / len(pieces))
        return jnp.repeat(jnp.exp(heights), extent[axis_at] // shards_of).reshape((-1,) + (1,) * (len(extent) - axis_at - 1))

    gain = one(*pieces[0])
    for cut in pieces[1:]:
        gain = gain * one(*cut)
    return gain


def assign_block(stream_key, own, number, rows, count, top, limit, slope):
    sequence = jax.random.permutation(stream_key, count)
    packed, common = shares(count, rows * top, limit, slope, True), shares(count, rows * top, limit, slope, False)
    places = jnp.arange(count)

    def named(sizes, turn):
        used = int((sizes > 0).sum())
        fixed = max(1, used // 4)
        shifted = fixed + (places - fixed + turn * (used - fixed)) % max(1, count - fixed)
        return jnp.zeros((count,), jnp.int32).at[sequence[jnp.where(places < fixed, places, shifted)]].set(jnp.asarray(sizes, jnp.int32))

    sizes = jnp.where(number % 4 == 0, named(packed, number // 4), named(common, number - number // 4 - 1))
    mixed = jax.random.permutation(jax.random.fold_in(own, 3), count)
    source_of, sink = mixed[0:count // 2 * 2:2], mixed[1:count // 2 * 2:2]
    slack = jnp.minimum(sizes[source_of] - 1, limit - sizes[sink]) // 2
    slack = jnp.where((source_of == sequence[0]) | (sink == sequence[0]) | (sizes[sink] == 0), 0, jnp.maximum(slack, 0))
    shifted = jax.random.randint(jax.random.fold_in(own, 4), (count // 2,), 0, 1 << 20) % (slack + 1)
    sizes = sizes.at[source_of].add(-shifted).at[sink].add(shifted)
    members = jnp.searchsorted(jnp.cumsum(sizes), jnp.arange(rows * top), side="right").astype(jnp.int32)
    listing = members.reshape(top, rows).T
    listing = listing[jax.random.permutation(jax.random.fold_in(own, 1), rows)]
    turn = jax.random.randint(jax.random.fold_in(own, 2), (rows, 1), 0, top)
    return jnp.take_along_axis(listing, (jnp.arange(top)[None, :] + turn) % top, axis=1)


def shares(count, total, most, skew, full):
    portions = [(1 << 20) // math.isqrt(standing ** skew) + 1 for standing in range(1, count + 1)]
    largest = most if full else min(most, max(-(-total // count), total * portions[0] // sum(portions)))
    least = 1 if total - largest >= count - 1 else 0
    given, surplus = [largest] + [least] * (count - 1), total - largest - least * (count - 1)
    while surplus > 0:
        free = [i for i in range(1, count) if given[i] < largest] or [i for i in range(1, count) if given[i] < most]
        mass, left = sum([portions[i] for i in free]), surplus
        for i in free:
            addition = min(most - given[i], max(1, left * portions[i] // mass), surplus)
            given[i] = given[i] + addition
            surplus = surplus - addition
    return np.array(given)


def normal_values(own_key, shape, scale, bound, cuts=(), dtype=jnp.bfloat16):
    values = scale * jax.random.normal(own_key, shape, jnp.float32)
    if cuts:
        values = values * block_scale(own_key, shape, cuts, -0.22, 0.18)
    return jnp.clip(values, -bound, bound).astype(dtype)


def setup_inputs(seed: int = 0) -> dict:
    arg_keys = jax.random.split(jax.random.key(seed), 7)
    wavefunction = draw_wavefunction(jax.random.fold_in(arg_keys[6], 71), 0)
    left_env = draw_left_env(jax.random.fold_in(arg_keys[6], 71), 0)
    right_env = normal_values(arg_keys[2], (TERMS, M, M), M ** -0.5, 0.25, ((1, 4),))
    task_in = set_ends(jax.random.randint(arg_keys[3], (TASKS,), 0, SECTORS), jax.random.fold_in(arg_keys[3], 1), 0, SECTORS - 1).astype(jnp.int32)
    task_out_keys = jax.random.split(jax.random.fold_in(arg_keys[4], 1), TASKS // TASKS)
    task_out_turns = jax.random.permutation(jax.random.fold_in(arg_keys[4], 3), TASKS // TASKS)
    task_out = jax.vmap(lambda own, number: assign_block(jax.random.fold_in(arg_keys[4], 2), own, number, TASKS, SECTORS, 1, CAP, 2))(task_out_keys, task_out_turns).reshape((TASKS, 1))
    task_term = set_ends(jax.random.randint(arg_keys[5], (TASKS,), 0, TERMS), jax.random.fold_in(arg_keys[5], 1), 0, TERMS - 1).astype(jnp.int32)
    return dict(wavefunction=wavefunction, left_env=left_env, right_env=right_env, task_in=task_in, task_out=task_out, task_term=task_term)


def reference(wavefunction, left_env, right_env, task_in, task_out, task_term):
    def one_task(task_id, totals):
        source = lax.dynamic_index_in_dim(wavefunction, task_in[task_id], 0, keepdims=False)
        term_id = task_term[task_id]
        left_block = lax.dynamic_index_in_dim(left_env, term_id, 0, keepdims=False).astype(jnp.float32)
        right_block = lax.dynamic_index_in_dim(right_env, term_id, 0, keepdims=False).astype(jnp.float32)
        high_part = lax.optimization_barrier(source.astype(jnp.bfloat16))
        low_part = (source - high_part.astype(jnp.float32)).astype(jnp.bfloat16)
        split_sum = high_part.astype(jnp.float32) + low_part.astype(jnp.float32)
        mixed_sum = jnp.dot(split_sum, right_block, precision=lax.Precision.HIGHEST)
        top_part = lax.optimization_barrier(mixed_sum.astype(jnp.bfloat16))
        rest_part = (mixed_sum - top_part.astype(jnp.float32)).astype(jnp.bfloat16)
        joined = top_part.astype(jnp.float32) + rest_part.astype(jnp.float32)
        result = jnp.dot(left_block, joined, precision=lax.Precision.HIGHEST)
        target = task_out[task_id, 0]
        current = lax.dynamic_index_in_dim(totals, target, 0, keepdims=True)
        return lax.dynamic_update_index_in_dim(totals, current + result[None], target, 0)

    start_totals = jnp.zeros((SECTORS, M, M), jnp.float32)
    return lax.fori_loop(0, TASKS, one_task, start_totals)
```

```python
import functools

import jax
import jax.numpy as jnp
from jax import lax
from jax.experimental import pallas as pl
from jax.experimental.pallas import tpu as pltpu
from jax.sharding import PartitionSpec as P


VMEM = pl.BlockSpec(memory_space=pltpu.VMEM)
SMEM = pl.BlockSpec(memory_space=pltpu.SMEM)
ANY = pl.BlockSpec(memory_space=pl.ANY)


def call(kernel, out_shape, in_specs, scratch=(), flops=1, moved=1, name=None):
    return pl.pallas_call(
        kernel,
        out_shape=out_shape,
        in_specs=in_specs,
        out_specs=jax.tree.map(lambda _: VMEM, out_shape),
        scratch_shapes=list(scratch),
        cost_estimate=pl.CostEstimate(flops=flops, bytes_accessed=moved, transcendentals=0),
        name=name,
    )


def pick_terms_kernel(base, me, count, term_ref, left_ref, right_ref, *rest):
    outs, sem = rest[:count], rest[count]
    copies = []
    start, mine = base(), me()
    for step in range(count):
        term = term_ref[start + lax.rem(mine + step, count)]
        copies.append(pltpu.make_async_copy(left_ref.at[term], outs[step].at[0], sem.at[2 * step]))
        copies.append(pltpu.make_async_copy(right_ref.at[term], outs[step].at[1], sem.at[2 * step + 1]))
    for copy in copies:
        copy.start()
    for copy in copies:
        copy.wait()


def partner_psi_kernel(base, sec, count, chips, in_ref, *rest):
    held, out = rest[:chips], rest[chips]
    start = base()
    chip, core = sec() // 2, lax.rem(sec(), 2)
    for slot in range(count):
        source = in_ref[start + slot]
        for step in range(chips):
            @pl.when((source // 2 == chip ^ step) & (lax.rem(source, 2) == core))
            def _():
                out[slot] = held[step][...]


def own_psi_kernel(base, sec, me, count, chips, in_ref, *rest):
    held, paired, outs = rest[:chips], rest[chips], rest[chips + 1 :]
    start, mine = base(), me()
    chip, core = sec() // 2, lax.rem(sec(), 2)
    for step in range(count):
        slot = lax.rem(mine + step, count)
        source = in_ref[start + slot]
        same = lax.rem(source, 2) == core
        for hop in range(chips):
            @pl.when((source // 2 == chip ^ hop) & same)
            def _():
                outs[step][...] = held[hop][...]

        @pl.when(jnp.logical_not(same))
        def _():
            outs[step][...] = paired[slot]


def task_kernel(me, count, *refs):
    envs, psis, outs = refs[:count], refs[count : 2 * count], refs[2 * count : 3 * count]
    high, low, right = refs[3 * count :]
    rows = psis[0].shape[0]
    mine = me()
    for step in range(count):
        place = pl.ds(pl.multiple_of(lax.rem(mine + count - step, count) * rows, rows), rows)
        right[place, :] = envs[step][1]
        psi = psis[step][...]
        top = psi.astype(jnp.bfloat16)
        high[place, :] = top
        low[place, :] = (psi - top.astype(jnp.float32)).astype(jnp.bfloat16)
    mixed = jnp.dot(high[...], right[...], preferred_element_type=jnp.float32) + jnp.dot(
        low[...], right[...], preferred_element_type=jnp.float32
    )
    top = mixed.astype(jnp.bfloat16)
    high[...] = top
    low[...] = (mixed - top.astype(jnp.float32)).astype(jnp.bfloat16)
    for step in range(count):
        left = envs[(count - step) % count][0]
        outs[step][...] = jnp.dot(left, high[...], preferred_element_type=jnp.float32) + jnp.dot(
            left, low[...], preferred_element_type=jnp.float32
        )


def combine_kernel(base, sec, me, count, chips, target_ref, *rest):
    parts, keeps, send = rest[:count], rest[count : count + chips], rest[count + chips]
    start, mine = base(), me()
    chip, core = sec() // 2, lax.rem(sec(), 2)
    targets = [target_ref[start + lax.rem(mine + count - step, count)] for step in range(count)]
    for hop in range(chips):
        for out, owner in ((keeps[hop], core), (send.at[hop], 1 - core)):
            wanted = (chip ^ hop) * 2 + owner
            total = jnp.zeros(parts[0].shape, jnp.float32)
            for step in range(count):
                total = total + jnp.where(targets[step] == wanted, parts[step][...], 0.0)
            out[...] = total


def body(wavefunction, left_env, right_env, task_in, task_out, task_term):
    groups, count = lax.axis_size("sec"), lax.axis_size("env")
    chips = groups // 2
    _, rows, cols = wavefunction.shape
    per_device = task_in.shape[0] // (groups * count)
    targets = task_out[:, 0]
    f32, bf16 = jnp.float32, jnp.bfloat16
    block = jax.ShapeDtypeStruct((rows, cols), f32)
    sec = lambda: lax.axis_index("sec")
    me = lambda: lax.axis_index("env")

    def along(shift):
        return [(i, (i + shift) % count) for i in range(count)]

    def across(hop):
        return [(i, i ^ (2 * hop)) for i in range(groups)]

    pair = [(i, i ^ 1) for i in range(groups)]
    psi = wavefunction[0]
    held = [psi] + [lax.ppermute(psi, "sec", across(hop)) for hop in range(1, chips)]

    keeps, sends = None, None
    for turn in range(per_device):
        base = lambda: (sec() * per_device + turn) * count
        partner_base = lambda: ((sec() ^ 1) * per_device + turn) * count
        env_block = jax.ShapeDtypeStruct((2, rows, cols), bf16)
        envs = call(
            functools.partial(pick_terms_kernel, base, me, count),
            [env_block] * count,
            [SMEM, ANY, ANY],
            [pltpu.SemaphoreType.DMA((2 * count,))],
            name="pick_terms",
        )(task_term, left_env, right_env)
        envs = [envs[0]] + [lax.ppermute(envs[s], "env", along(s)) for s in range(1, count)]
        sent = call(
            functools.partial(partner_psi_kernel, partner_base, sec, count, chips),
            jax.ShapeDtypeStruct((count, rows, cols), f32),
            [SMEM] + [VMEM] * chips,
            name="partner_psi",
        )(task_in, *held)
        paired = lax.ppermute(sent, "sec", pair)
        psis = call(
            functools.partial(own_psi_kernel, base, sec, me, count, chips),
            [block] * count,
            [SMEM] + [VMEM] * (chips + 1),
            name="own_psi",
        )(task_in, *held, paired)
        psis = [psis[0]] + [lax.ppermute(psis[s], "env", along(s)) for s in range(1, count)]
        full = count * rows
        parts = call(
            functools.partial(task_kernel, me, count),
            [block] * count,
            [VMEM] * (2 * count),
            [pltpu.VMEM((full, cols), bf16)] * 3,
            flops=8 * full * full * cols,
            name="task",
        )(*envs, *psis)
        parts = [parts[0]] + [lax.ppermute(parts[s], "env", along(s)) for s in range(1, count)]
        *kept, send = call(
            functools.partial(combine_kernel, base, sec, me, count, chips),
            [block] * chips + [jax.ShapeDtypeStruct((chips, rows, cols), f32)],
            [SMEM] + [VMEM] * count,
            name="combine",
        )(targets, *parts)
        keeps = kept if keeps is None else [a + b for a, b in zip(keeps, kept)]
        sends = send if sends is None else sends + send
    other = lax.ppermute(sends, "sec", pair)
    sums = [keeps[hop] + other[hop] for hop in range(chips)]
    total = sums[0]
    for hop in range(1, chips):
        total = total + lax.ppermute(sums[hop], "sec", across(hop))
    return total[None]


def solution(mesh):
    placed = (P("sec", "env", None), P(None, "env", None), P(None, "env", None), P(), P(), P())
    return jax.shard_map(
        body, mesh=mesh, in_specs=placed, out_specs=P("sec", "env", None), check_vma=False
    )
```

```python
import functools

import jax
import jax.numpy as jnp
from jax import lax
from jax.experimental import pallas as pl
from jax.experimental.pallas import tpu as pltpu
from jax.sharding import PartitionSpec as P


VMEM_BYTES = 16 * 1024 * 1024
VMEM = pl.BlockSpec(memory_space=pltpu.VMEM)
SMEM = pl.BlockSpec(memory_space=pltpu.SMEM)
HBM = pl.BlockSpec(memory_space=pltpu.HBM)


def call(kernel, out_shape, in_specs, scratch=(), flops=1, moved=1):
    return pl.pallas_call(
        kernel,
        out_shape=out_shape,
        in_specs=in_specs,
        out_specs=jax.tree.map(lambda _: VMEM, out_shape),
        scratch_shapes=list(scratch),
        cost_estimate=pl.CostEstimate(flops=flops, bytes_accessed=moved, transcendentals=0),
        compiler_params=pltpu.CompilerParams(vmem_limit_bytes=VMEM_BYTES),
    )


def pick_terms_kernel(base, me, count, term_ref, left_ref, right_ref, *rest):
    outs, sem = rest[:count], rest[count]
    copies = []
    start, mine = base(), me()
    for step in range(count):
        term = term_ref[start + lax.rem(mine + step, count)]
        copies.append(pltpu.make_async_copy(left_ref.at[term], outs[step].at[0], sem.at[2 * step]))
        copies.append(pltpu.make_async_copy(right_ref.at[term], outs[step].at[1], sem.at[2 * step + 1]))
    for copy in copies:
        copy.start()
    for copy in copies:
        copy.wait()


def partner_psi_kernel(base, sec, count, chips, in_ref, *rest):
    held, out = rest[:chips], rest[chips]
    start = base()
    chip, core = sec() // 2, lax.rem(sec(), 2)
    for slot in range(count):
        source = in_ref[start + slot]
        for step in range(chips):
            @pl.when((source // 2 == chip ^ step) & (lax.rem(source, 2) == core))
            def _():
                out[slot] = held[step][...]


def own_psi_kernel(base, sec, me, count, chips, in_ref, *rest):
    held, paired, outs = rest[:chips], rest[chips], rest[chips + 1 :]
    start, mine = base(), me()
    chip, core = sec() // 2, lax.rem(sec(), 2)
    for step in range(count):
        slot = lax.rem(mine + step, count)
        source = in_ref[start + slot]
        same = lax.rem(source, 2) == core
        for hop in range(chips):
            @pl.when((source // 2 == chip ^ hop) & same)
            def _():
                outs[step][...] = held[hop][...]

        @pl.when(jnp.logical_not(same))
        def _():
            outs[step][...] = paired[slot]


def task_kernel(me, count, *refs):
    envs, psis, outs = refs[:count], refs[count : 2 * count], refs[2 * count : 3 * count]
    high, low, right = refs[3 * count :]
    rows = psis[0].shape[0]
    mine = me()
    for step in range(count):
        place = pl.ds(pl.multiple_of(lax.rem(mine + count - step, count) * rows, rows), rows)
        right[place, :] = envs[step][1]
        psi = psis[step][...]
        top = psi.astype(jnp.bfloat16)
        high[place, :] = top
        low[place, :] = (psi - top.astype(jnp.float32)).astype(jnp.bfloat16)
    mixed = jnp.dot(high[...], right[...], preferred_element_type=jnp.float32) + jnp.dot(
        low[...], right[...], preferred_element_type=jnp.float32
    )
    top = mixed.astype(jnp.bfloat16)
    high[...] = top
    low[...] = (mixed - top.astype(jnp.float32)).astype(jnp.bfloat16)
    for step in range(count):
        left = envs[(count - step) % count][0]
        outs[step][...] = jnp.dot(left, high[...], preferred_element_type=jnp.float32) + jnp.dot(
            left, low[...], preferred_element_type=jnp.float32
        )


def combine_kernel(base, sec, me, count, chips, target_ref, *rest):
    parts, keeps, send = rest[:count], rest[count : count + chips], rest[count + chips]
    start, mine = base(), me()
    chip, core = sec() // 2, lax.rem(sec(), 2)
    targets = [target_ref[start + lax.rem(mine + count - step, count)] for step in range(count)]
    for hop in range(chips):
        for out, owner in ((keeps[hop], core), (send.at[hop], 1 - core)):
            wanted = (chip ^ hop) * 2 + owner
            total = jnp.zeros(parts[0].shape, jnp.float32)
            for step in range(count):
                total = total + jnp.where(targets[step] == wanted, parts[step][...], 0.0)
            out[...] = total


def body(wavefunction, left_env, right_env, task_in, task_out, task_term):
    groups, count = lax.axis_size("sec"), lax.axis_size("env")
    chips = groups // 2
    _, rows, cols = wavefunction.shape
    per_device = task_in.shape[0] // (groups * count)
    targets = task_out[:, 0]
    f32, bf16 = jnp.float32, jnp.bfloat16
    block = jax.ShapeDtypeStruct((rows, cols), f32)
    sec = lambda: lax.axis_index("sec")
    me = lambda: lax.axis_index("env")

    def along(shift):
        return [(i, (i + shift) % count) for i in range(count)]

    def across(hop):
        return [(i, i ^ (2 * hop)) for i in range(groups)]

    pair = [(i, i ^ 1) for i in range(groups)]
    psi = wavefunction[0]
    held = [psi] + [lax.ppermute(psi, "sec", across(hop)) for hop in range(1, chips)]

    keeps, sends = None, None
    for turn in range(per_device):
        base = lambda: (sec() * per_device + turn) * count
        partner_base = lambda: ((sec() ^ 1) * per_device + turn) * count
        env_block = jax.ShapeDtypeStruct((2, rows, cols), bf16)
        envs = call(
            functools.partial(pick_terms_kernel, base, me, count),
            [env_block] * count,
            [SMEM, HBM, HBM],
            [pltpu.SemaphoreType.DMA((2 * count,))],
        )(task_term, left_env, right_env)
        envs = [envs[0]] + [lax.ppermute(envs[s], "env", along(s)) for s in range(1, count)]
        sent = call(
            functools.partial(partner_psi_kernel, partner_base, sec, count, chips),
            jax.ShapeDtypeStruct((count, rows, cols), f32),
            [SMEM] + [VMEM] * chips,
        )(task_in, *held)
        paired = lax.ppermute(sent, "sec", pair)
        psis = call(
            functools.partial(own_psi_kernel, base, sec, me, count, chips),
            [block] * count,
            [SMEM] + [VMEM] * (chips + 1),
        )(task_in, *held, paired)
        psis = [psis[0]] + [lax.ppermute(psis[s], "env", along(s)) for s in range(1, count)]
        full = count * rows
        parts = call(
            functools.partial(task_kernel, me, count),
            [block] * count,
            [VMEM] * (2 * count),
            [pltpu.VMEM((full, cols), bf16)] * 3,
            flops=8 * full * full * cols,
        )(*envs, *psis)
        parts = [parts[0]] + [lax.ppermute(parts[s], "env", along(s)) for s in range(1, count)]
        *kept, send = call(
            functools.partial(combine_kernel, base, sec, me, count, chips),
            [block] * chips + [jax.ShapeDtypeStruct((chips, rows, cols), f32)],
            [SMEM] + [VMEM] * count,
        )(targets, *parts)
        keeps = kept if keeps is None else [a + b for a, b in zip(keeps, kept)]
        sends = send if sends is None else sends + send
    other = lax.ppermute(sends, "sec", pair)
    sums = [keeps[hop] + other[hop] for hop in range(chips)]
    total = sums[0]
    for hop in range(1, chips):
        total = total + lax.ppermute(sums[hop], "sec", across(hop))
    return total[None]


def solution(mesh):
    placed = (P("sec", "env", None), P(None, "env", None), P(None, "env", None), P(), P(), P())
    return jax.shard_map(
        body, mesh=mesh, in_specs=placed, out_specs=P("sec", "env", None), check_vma=False
    )
```

```python
import functools

import jax
import jax.numpy as jnp
from jax import lax
from jax.experimental import pallas as pl
from jax.experimental.pallas import tpu as pltpu
from jax.sharding import PartitionSpec as P


GRID, LIMIT, LEVELS, HEAD = 1024.0, 32767.0, 256.0, 16
PREPARE_BYTES = 63_400_000
VMEM_BYTES = 16 * 1024 * 1024
VMEM = pl.BlockSpec(memory_space=pltpu.VMEM)
SMEM = pl.BlockSpec(memory_space=pltpu.SMEM)
HBM = pl.BlockSpec(memory_space=pltpu.HBM)


def call(kernel, out_shape, in_specs, scratch=(), flops=1, vmem=VMEM_BYTES):
    return pl.pallas_call(
        kernel,
        out_shape=out_shape,
        in_specs=in_specs,
        out_specs=jax.tree.map(lambda _: VMEM, out_shape),
        scratch_shapes=list(scratch),
        cost_estimate=pl.CostEstimate(flops=flops, bytes_accessed=1, transcendentals=0),
        compiler_params=pltpu.CompilerParams(vmem_limit_bytes=vmem),
    )


def encode(value, out, centred):
    rows = value.shape[0]
    centre = jnp.zeros_like(value[:1])
    if centred:
        middle = (jnp.max(value, axis=0, keepdims=True) + jnp.min(value, axis=0, keepdims=True)) / 2
        centre = jnp.clip((middle * GRID).astype(jnp.int32), -LIMIT, LIMIT).astype(jnp.float32)
        value = value - centre / GRID
    span = jnp.max(jnp.abs(value), axis=0, keepdims=True)
    level = jnp.log(jnp.maximum(span, 1e-30)) * LEVELS + 1.0
    level = (level + jnp.where(level > 0, 1.0, 0.0)).astype(jnp.int32).astype(jnp.float32)
    scaled = value * (LIMIT / jnp.exp(level / LEVELS))
    scaled = jnp.clip(scaled + jnp.where(scaled > 0, 0.5, -0.5), -LIMIT, LIMIT)
    out[pl.ds(0, rows), :] = scaled.astype(jnp.int32).astype(jnp.int16)
    lines = lax.broadcasted_iota(jnp.int32, (HEAD, value.shape[1]), 0)
    head = jnp.where(lines == 0, level.astype(jnp.int32), centre.astype(jnp.int32))
    out[pl.ds(rows, HEAD), :] = head.astype(jnp.int16)


def decode(code):
    rows = code.shape[0] - HEAD
    head = code[pl.ds(rows, HEAD), :].astype(jnp.int32).astype(jnp.float32)
    step = jnp.exp(head[0:1] / LEVELS) / LIMIT
    value = code[pl.ds(0, rows), :].astype(jnp.int32).astype(jnp.float32)
    return value * step + head[1:2] / GRID


def prepare_kernel(base, me, count, term_ref, psi_ref, left_ref, right_ref, *rest):
    outs, code, sem = rest[:count], rest[count], rest[count + 1]
    copies = []
    start, mine = base(), me()
    for step in range(count):
        term = term_ref[start + lax.rem(mine + step, count)]
        copies.append(pltpu.make_async_copy(left_ref.at[term], outs[step].at[0], sem.at[2 * step]))
        copies.append(pltpu.make_async_copy(right_ref.at[term], outs[step].at[1], sem.at[2 * step + 1]))
    for copy in copies:
        copy.start()
    encode(psi_ref[...], code, True)
    for copy in copies:
        copy.wait()


def partner_psi_kernel(base, sec, count, chips, in_ref, *rest):
    held, out = rest[:chips], rest[chips]
    start = base()
    chip, core = sec() // 2, lax.rem(sec(), 2)
    for slot in range(count):
        source = in_ref[start + slot]
        for step in range(chips):
            @pl.when((source // 2 == chip ^ step) & (lax.rem(source, 2) == core))
            def _():
                out[slot] = held[step][...]


def own_psi_kernel(base, sec, me, count, chips, in_ref, *rest):
    held, paired, outs = rest[:chips], rest[chips], rest[chips + 1 :]
    start, mine = base(), me()
    chip, core = sec() // 2, lax.rem(sec(), 2)
    for step in range(count):
        slot = lax.rem(mine + step, count)
        source = in_ref[start + slot]
        same = lax.rem(source, 2) == core
        for hop in range(chips):
            @pl.when((source // 2 == chip ^ hop) & same)
            def _():
                outs[step][...] = held[hop][...]

        @pl.when(jnp.logical_not(same))
        def _():
            outs[step][...] = paired[slot]


def task_kernel(me, count, *refs):
    envs, psis, outs = refs[:count], refs[count : 2 * count], refs[2 * count : 3 * count]
    high, low, right = refs[3 * count :]
    rows = outs[0].shape[0]
    mine = me()
    for step in range(count):
        place = pl.ds(pl.multiple_of(lax.rem(mine + count - step, count) * rows, rows), rows)
        right[place, :] = envs[step][1]
        psi = decode(psis[step])
        top = psi.astype(jnp.bfloat16)
        high[place, :] = top
        low[place, :] = (psi - top.astype(jnp.float32)).astype(jnp.bfloat16)
    mixed = jnp.dot(high[...], right[...], preferred_element_type=jnp.float32) + jnp.dot(
        low[...], right[...], preferred_element_type=jnp.float32
    )
    top = mixed.astype(jnp.bfloat16)
    high[...] = top
    low[...] = (mixed - top.astype(jnp.float32)).astype(jnp.bfloat16)
    for step in range(count):
        left = envs[(count - step) % count][0]
        part = jnp.dot(left, high[...], preferred_element_type=jnp.float32) + jnp.dot(
            left, low[...], preferred_element_type=jnp.float32
        )
        if step == 0:
            outs[0][...] = part
        else:
            encode(part, outs[step], False)


def combine_kernel(base, sec, me, count, target_ref, *rest):
    parts, keep, send = rest[:count], rest[count], rest[count + 1]
    start, mine = base(), me()
    chip, core = sec() // 2, lax.rem(sec(), 2)
    keep[...] = jnp.zeros(keep.shape, jnp.float32)
    send[...] = jnp.zeros(send.shape, jnp.float32)
    for step in range(count):
        target = target_ref[start + lax.rem(mine + count - step, count)]
        hop = (target // 2) ^ chip
        part = parts[0][...] if step == 0 else decode(parts[step])
        mine_too = lax.rem(target, 2) == core

        @pl.when(mine_too)
        def _():
            keep[hop] = keep[hop] + part

        @pl.when(jnp.logical_not(mine_too))
        def _():
            send[hop] = send[hop] + part


def join_kernel(chips, keep, other, *outs):
    for hop in range(chips):
        total = keep[hop] + other[hop]
        if hop == 0:
            outs[0][...] = total
        else:
            encode(total, outs[hop], False)


def finish_kernel(chips, *refs):
    total = refs[0][...]
    for hop in range(1, chips):
        total = total + decode(refs[hop])
    refs[chips][...] = total


def body(wavefunction, left_env, right_env, task_in, task_out, task_term):
    groups, count = lax.axis_size("sec"), lax.axis_size("env")
    chips = groups // 2
    _, rows, cols = wavefunction.shape
    per_device = task_in.shape[0] // (groups * count)
    targets = task_out[:, 0]
    f32, bf16 = jnp.float32, jnp.bfloat16
    block = jax.ShapeDtypeStruct((rows, cols), f32)
    sec = lambda: lax.axis_index("sec")
    me = lambda: lax.axis_index("env")

    def along(shift):
        return [(i, (i + shift) % count) for i in range(count)]

    def across(hop):
        return [(i, i ^ (2 * hop)) for i in range(groups)]

    pair = [(i, i ^ 1) for i in range(groups)]
    code = jax.ShapeDtypeStruct((rows + HEAD, cols), jnp.int16)
    stack = jax.ShapeDtypeStruct((chips, rows, cols), f32)

    keep, send, held = None, None, None
    for turn in range(per_device):
        base = lambda: (sec() * per_device + turn) * count
        partner_base = lambda: ((sec() ^ 1) * per_device + turn) * count
        env_block = jax.ShapeDtypeStruct((2, rows, cols), bf16)
        *envs, psi = call(
            functools.partial(prepare_kernel, base, me, count),
            [env_block] * count + [code],
            [SMEM, VMEM, HBM, HBM],
            [pltpu.SemaphoreType.DMA((2 * count,))],
            vmem=PREPARE_BYTES,
        )(task_term, wavefunction[0], left_env, right_env)
        envs = [envs[0]] + [lax.ppermute(envs[s], "env", along(s)) for s in range(1, count)]
        if held is None:
            held = [psi] + [lax.ppermute(psi, "sec", across(hop)) for hop in range(1, chips)]
        sent = call(
            functools.partial(partner_psi_kernel, partner_base, sec, count, chips),
            jax.ShapeDtypeStruct((count, *code.shape), code.dtype),
            [SMEM] + [VMEM] * chips,
        )(task_in, *held)
        paired = lax.ppermute(sent, "sec", pair)
        psis = call(
            functools.partial(own_psi_kernel, base, sec, me, count, chips),
            [code] * count,
            [SMEM] + [VMEM] * (chips + 1),
        )(task_in, *held, paired)
        psis = [psis[0]] + [lax.ppermute(psis[s], "env", along(s)) for s in range(1, count)]
        full = count * rows
        parts = call(
            functools.partial(task_kernel, me, count),
            [block] + [code] * (count - 1),
            [VMEM] * (2 * count),
            [pltpu.VMEM((full, cols), bf16)] * 3,
            flops=8 * full * full * cols,
        )(*envs, *psis)
        parts = [parts[0]] + [lax.ppermute(parts[s], "env", along(s)) for s in range(1, count)]
        kept, sends = call(
            functools.partial(combine_kernel, base, sec, me, count),
            [stack, stack],
            [SMEM] + [VMEM] * count,
        )(targets, *parts)
        keep = kept if keep is None else keep + kept
        send = sends if send is None else send + sends
    other = lax.ppermute(send, "sec", pair)
    sums = call(
        functools.partial(join_kernel, chips), [block] + [code] * (chips - 1), [VMEM] * 2
    )(keep, other)
    sums = [sums[0]] + [lax.ppermute(sums[hop], "sec", across(hop)) for hop in range(1, chips)]
    total = call(functools.partial(finish_kernel, chips), block, [VMEM] * chips)(*sums)
    return total[None]


def solution(mesh):
    placed = (P("sec", "env", None), P(None, "env", None), P(None, "env", None), P(), P(), P())
    return jax.shard_map(
        body, mesh=mesh, in_specs=placed, out_specs=P("sec", "env", None), check_vma=False
    )
```

```python
import functools

import jax
import jax.numpy as jnp
from jax import lax
from jax.experimental import pallas as pl
from jax.experimental.pallas import tpu as pltpu
from jax.sharding import PartitionSpec as P


GRID, LIMIT, LEVELS, HEAD, HALVES = 1024.0, 32767.0, 256.0, 8, 2
PREPARE_BYTES = 52_000_000
VMEM_BYTES = 16 * 1024 * 1024
VMEM = pl.BlockSpec(memory_space=pltpu.VMEM)
SMEM = pl.BlockSpec(memory_space=pltpu.SMEM)
HBM = pl.BlockSpec(memory_space=pltpu.HBM)


def call(kernel, out_shape, in_specs, scratch=(), flops=1, vmem=VMEM_BYTES):
    return pl.pallas_call(
        kernel,
        out_shape=out_shape,
        in_specs=in_specs,
        out_specs=jax.tree.map(lambda _: VMEM, out_shape),
        scratch_shapes=list(scratch),
        cost_estimate=pl.CostEstimate(flops=flops, bytes_accessed=1, transcendentals=0),
        compiler_params=pltpu.CompilerParams(vmem_limit_bytes=vmem),
    )


def encode(value, out, centred):
    rows = value.shape[0]
    centre = jnp.zeros_like(value[:1])
    if centred:
        middle = (jnp.max(value, axis=0, keepdims=True) + jnp.min(value, axis=0, keepdims=True)) / 2
        centre = jnp.clip((middle * GRID).astype(jnp.int32), -LIMIT, LIMIT).astype(jnp.float32)
        value = value - centre / GRID
    span = jnp.max(jnp.abs(value), axis=0, keepdims=True)
    level = jnp.log(jnp.maximum(span, 1e-30)) * LEVELS + 1.0
    level = (level + jnp.where(level > 0, 1.0, 0.0)).astype(jnp.int32).astype(jnp.float32)
    scaled = value * (LIMIT / jnp.exp(level / LEVELS))
    scaled = jnp.clip(scaled + jnp.where(scaled > 0, 0.5, -0.5), -LIMIT, LIMIT)
    out[pl.ds(0, rows), :] = scaled.astype(jnp.int32).astype(jnp.int16)
    lines = lax.broadcasted_iota(jnp.int32, (HEAD, value.shape[1]), 0)
    head = jnp.where(lines == 0, level.astype(jnp.int32), centre.astype(jnp.int32))
    out[pl.ds(rows, HEAD), :] = head.astype(jnp.int16)


def decode(code):
    rows = code.shape[0] - HEAD
    head = code[pl.ds(rows, HEAD), :].astype(jnp.int32).astype(jnp.float32)
    step = jnp.exp(head[0:1] / LEVELS) / LIMIT
    value = code[pl.ds(0, rows), :].astype(jnp.int32).astype(jnp.float32)
    return value * step + head[1:2] / GRID


def prepare_kernel(base, me, count, term_ref, psi_ref, left_ref, right_ref, *rest):
    outs, code, sem = rest[:count], rest[count], rest[count + 1]
    copies = []
    start, mine = base(), me()
    for step in range(count):
        term = term_ref[start + mine ^ step]
        copies.append(pltpu.make_async_copy(left_ref.at[term], outs[step].at[0], sem.at[2 * step]))
        copies.append(pltpu.make_async_copy(right_ref.at[term], outs[step].at[1], sem.at[2 * step + 1]))
    for copy in copies:
        copy.start()
    encode(psi_ref[...], code, True)
    for copy in copies:
        copy.wait()


def partner_psi_kernel(base, sec, count, chips, in_ref, *rest):
    held, out = rest[:chips], rest[chips]
    start = base()
    chip, core = sec() // 2, lax.rem(sec(), 2)
    for slot in range(count):
        source = in_ref[start + slot]
        for step in range(chips):
            @pl.when((source // 2 == chip ^ step) & (lax.rem(source, 2) == core))
            def _():
                out[slot] = held[step][...]


def own_psi_kernel(base, sec, me, count, chips, in_ref, *rest):
    held, paired, outs = rest[:chips], rest[chips], rest[chips + 1 :]
    start, mine = base(), me()
    chip, core = sec() // 2, lax.rem(sec(), 2)
    for step in range(count):
        slot = mine ^ step
        source = in_ref[start + slot]
        same = lax.rem(source, 2) == core
        for hop in range(chips):
            @pl.when((source // 2 == chip ^ hop) & same)
            def _():
                outs[step][...] = held[hop][...]

        @pl.when(jnp.logical_not(same))
        def _():
            outs[step][...] = paired[slot]


def task_kernel(me, count, *refs):
    envs, psis, outs = refs[:count], refs[count : 2 * count], refs[2 * count : -3]
    high, low, right = refs[-3:]
    rows, width = outs[0].shape
    mine = me()
    for step in range(count):
        place = pl.ds(pl.multiple_of((mine ^ step) * rows, rows), rows)
        right[place, :] = envs[step][1]
        psi = decode(psis[step])
        top = psi.astype(jnp.bfloat16)
        high[place, :] = top
        low[place, :] = (psi - top.astype(jnp.float32)).astype(jnp.bfloat16)
    mixed = jnp.dot(high[...], right[...], preferred_element_type=jnp.float32) + jnp.dot(
        low[...], right[...], preferred_element_type=jnp.float32
    )
    top = mixed.astype(jnp.bfloat16)
    high[...] = top
    low[...] = (mixed - top.astype(jnp.float32)).astype(jnp.bfloat16)
    for step in range(count):
        left = envs[step][0]
        part = jnp.dot(left, high[...], preferred_element_type=jnp.float32) + jnp.dot(
            left, low[...], preferred_element_type=jnp.float32
        )
        for half in range(HALVES):
            piece, out = part[:, half * width : (half + 1) * width], outs[half * count + step]
            if step == 0:
                out[...] = piece
            else:
                encode(piece, out, False)


def combine_kernel(base, sec, me, count, target_ref, *rest):
    parts, keep, send = rest[:count], rest[count], rest[count + 1]
    start, mine = base(), me()
    chip, core = sec() // 2, lax.rem(sec(), 2)
    keep[...] = jnp.zeros(keep.shape, jnp.float32)
    send[...] = jnp.zeros(send.shape, jnp.float32)
    for step in range(count):
        target = target_ref[start + mine ^ step]
        hop = (target // 2) ^ chip
        part = parts[0][...] if step == 0 else decode(parts[step])
        mine_too = lax.rem(target, 2) == core

        @pl.when(mine_too)
        def _():
            keep[hop] = keep[hop] + part

        @pl.when(jnp.logical_not(mine_too))
        def _():
            send[hop] = send[hop] + part


def join_kernel(chips, keep, other, *outs):
    for hop in range(chips):
        total = keep[hop] + other[hop]
        if hop == 0:
            outs[0][...] = total
        else:
            encode(total, outs[hop], False)


def finish_kernel(chips, *refs):
    width = refs[0].shape[1]
    for half in range(HALVES):
        mine = refs[half * chips : (half + 1) * chips]
        total = mine[0][...]
        for hop in range(1, chips):
            total = total + decode(mine[hop])
        refs[-1][:, half * width : (half + 1) * width] = total


def body(wavefunction, left_env, right_env, task_in, task_out, task_term):
    groups, count = lax.axis_size("sec"), lax.axis_size("env")
    chips = groups // 2
    _, rows, cols = wavefunction.shape
    per_device = task_in.shape[0] // (groups * count)
    targets = task_out[:, 0]
    f32, bf16 = jnp.float32, jnp.bfloat16
    block = jax.ShapeDtypeStruct((rows, cols), f32)
    sec = lambda: lax.axis_index("sec")
    me = lambda: lax.axis_index("env")

    def along(shift):
        return [(i, i ^ shift) for i in range(count)]

    def across(hop):
        return [(i, i ^ (2 * hop)) for i in range(groups)]

    pair = [(i, i ^ 1) for i in range(groups)]
    code = jax.ShapeDtypeStruct((rows + HEAD, cols), jnp.int16)
    width = cols // HALVES
    part = jax.ShapeDtypeStruct((rows, width), f32)
    piece = jax.ShapeDtypeStruct((rows + HEAD, width), jnp.int16)
    stack = jax.ShapeDtypeStruct((chips, rows, width), f32)

    keeps, sends, held = [None] * HALVES, [None] * HALVES, None
    for turn in range(per_device):
        base = lambda: (sec() * per_device + turn) * count
        partner_base = lambda: ((sec() ^ 1) * per_device + turn) * count
        env_block = jax.ShapeDtypeStruct((2, rows, cols), bf16)
        *envs, psi = call(
            functools.partial(prepare_kernel, base, me, count),
            [env_block] * count + [code],
            [SMEM, VMEM, HBM, HBM],
            [pltpu.SemaphoreType.DMA((2 * count,))],
            vmem=PREPARE_BYTES,
        )(task_term, wavefunction[0], left_env, right_env)
        envs = [envs[0]] + [lax.ppermute(envs[s], "env", along(s)) for s in range(1, count)]
        if held is None:
            held = [psi] + [lax.ppermute(psi, "sec", across(hop)) for hop in range(1, chips)]
        sent = call(
            functools.partial(partner_psi_kernel, partner_base, sec, count, chips),
            jax.ShapeDtypeStruct((count, *code.shape), code.dtype),
            [SMEM] + [VMEM] * chips,
        )(task_in, *held)
        paired = lax.ppermute(sent, "sec", pair)
        psis = call(
            functools.partial(own_psi_kernel, base, sec, me, count, chips),
            [code] * count,
            [SMEM] + [VMEM] * (chips + 1),
        )(task_in, *held, paired)
        psis = [psis[0]] + [lax.ppermute(psis[s], "env", along(s)) for s in range(1, count)]
        full = count * rows
        parts = call(
            functools.partial(task_kernel, me, count),
            ([part] + [piece] * (count - 1)) * HALVES,
            [VMEM] * (2 * count),
            [pltpu.VMEM((full, cols), bf16)] * 3,
            flops=8 * full * full * cols,
        )(*envs, *psis)
        halves = [parts[half * count : (half + 1) * count] for half in range(HALVES)]
        halves = [
            [mine[0]] + [lax.ppermute(mine[s], "env", along(s)) for s in range(1, count)]
            for mine in halves
        ]
        for half, mine in enumerate(halves):
            kept, sent = call(
                functools.partial(combine_kernel, base, sec, me, count),
                [stack, stack],
                [SMEM] + [VMEM] * count,
            )(targets, *mine)
            if turn:
                kept, sent = keeps[half] + kept, sends[half] + sent
            keeps[half], sends[half] = kept, sent
    sums = []
    for half in range(HALVES):
        other = lax.ppermute(sends[half], "sec", pair)
        mine = call(
            functools.partial(join_kernel, chips), [part] + [piece] * (chips - 1), [VMEM] * 2
        )(keeps[half], other)
        sums += [mine[0]]
        sums += [lax.ppermute(mine[hop], "sec", across(hop)) for hop in range(1, chips)]
    total = call(functools.partial(finish_kernel, chips), block, [VMEM] * (chips * HALVES))(*sums)
    return total[None]


def solution(mesh):
    placed = (P("sec", "env", None), P(None, "env", None), P(None, "env", None), P(), P(), P())
    return jax.shard_map(
        body, mesh=mesh, in_specs=placed, out_specs=P("sec", "env", None), check_vma=False
    )
```

```python
import functools

import jax
import jax.numpy as jnp
from jax import lax
from jax.experimental import pallas as pl
from jax.experimental.pallas import tpu as pltpu
from jax.sharding import PartitionSpec as P


GRID, LIMIT, LEVELS, HEAD, HALVES = 1024.0, 32767.0, 256.0, 8, 1
PICK_BYTES = 54_000_000
VMEM_BYTES = 16 * 1024 * 1024
VMEM = pl.BlockSpec(memory_space=pltpu.VMEM)
SMEM = pl.BlockSpec(memory_space=pltpu.SMEM)
HBM = pl.BlockSpec(memory_space=pltpu.HBM)


def call(kernel, out_shape, in_specs, scratch=(), flops=1, vmem=VMEM_BYTES):
    return pl.pallas_call(
        kernel,
        out_shape=out_shape,
        in_specs=in_specs,
        out_specs=jax.tree.map(lambda _: VMEM, out_shape),
        scratch_shapes=list(scratch),
        cost_estimate=pl.CostEstimate(flops=flops, bytes_accessed=1, transcendentals=0),
        compiler_params=pltpu.CompilerParams(vmem_limit_bytes=vmem),
    )


def encode(value, out, centred):
    rows = value.shape[0]
    centre = jnp.zeros_like(value[:1])
    if centred:
        middle = (jnp.max(value, axis=0, keepdims=True) + jnp.min(value, axis=0, keepdims=True)) / 2
        centre = jnp.clip((middle * GRID).astype(jnp.int32), -LIMIT, LIMIT).astype(jnp.float32)
        value = value - centre / GRID
    span = jnp.max(jnp.abs(value), axis=0, keepdims=True)
    level = jnp.log(jnp.maximum(span, 1e-30)) * LEVELS + 1.0
    level = (level + jnp.where(level > 0, 1.0, 0.0)).astype(jnp.int32).astype(jnp.float32)
    scaled = value * (LIMIT / jnp.exp(level / LEVELS))
    scaled = jnp.clip(scaled + jnp.where(scaled > 0, 0.5, -0.5), -LIMIT, LIMIT)
    out[pl.ds(0, rows), :] = scaled.astype(jnp.int32).astype(jnp.int16)
    lines = lax.broadcasted_iota(jnp.int32, (HEAD, value.shape[1]), 0)
    head = jnp.where(lines == 0, level.astype(jnp.int32), centre.astype(jnp.int32))
    out[pl.ds(rows, HEAD), :] = head.astype(jnp.int16)


def decode(code):
    rows = code.shape[0] - HEAD
    head = code[pl.ds(rows, HEAD), :].astype(jnp.int32).astype(jnp.float32)
    step = jnp.exp(head[0:1] / LEVELS) / LIMIT
    value = code[pl.ds(0, rows), :].astype(jnp.int32).astype(jnp.float32)
    return value * step + head[1:2] / GRID


def pick_kernel(base, me, count, term_ref, left_ref, right_ref, *rest):
    outs, sem = rest[:count], rest[count]
    copies = []
    start, mine = base(), me()
    for step in range(count):
        term = term_ref[start + (mine ^ step)]
        copies.append(pltpu.make_async_copy(left_ref.at[term], outs[step].at[0], sem.at[2 * step]))
        copies.append(pltpu.make_async_copy(right_ref.at[term], outs[step].at[1], sem.at[2 * step + 1]))
    for copy in copies:
        copy.start()
    for copy in copies:
        copy.wait()


def encode_kernel(psi_ref, code):
    encode(psi_ref[...], code, True)


def partner_psi_kernel(base, sec, count, chips, in_ref, *rest):
    held, out = rest[:chips], rest[chips]
    start = base()
    chip, core = sec() // 2, lax.rem(sec(), 2)
    for slot in range(count):
        source = in_ref[start + slot]
        for step in range(chips):
            @pl.when((source // 2 == chip ^ step) & (lax.rem(source, 2) == core))
            def _():
                out[slot] = held[step][...]


def own_psi_kernel(base, sec, me, count, chips, in_ref, *rest):
    held, paired, outs = rest[:chips], rest[chips], rest[chips + 1 :]
    start, mine = base(), me()
    chip, core = sec() // 2, lax.rem(sec(), 2)
    for step in range(count):
        slot = mine ^ step
        source = in_ref[start + slot]
        same = lax.rem(source, 2) == core
        for hop in range(chips):
            @pl.when((source // 2 == chip ^ hop) & same)
            def _():
                outs[step][...] = held[hop][...]

        @pl.when(jnp.logical_not(same))
        def _():
            outs[step][...] = paired[slot]


def task_kernel(me, count, *refs):
    envs, psis, outs = refs[:count], refs[count : 2 * count], refs[2 * count : -3]
    high, low, right = refs[-3:]
    rows, width = outs[0].shape
    mine = me()
    for step in range(count):
        place = pl.ds(pl.multiple_of((mine ^ step) * rows, rows), rows)
        right[place, :] = envs[step][1]
        psi = decode(psis[step])
        top = psi.astype(jnp.bfloat16)
        high[place, :] = top
        low[place, :] = (psi - top.astype(jnp.float32)).astype(jnp.bfloat16)
    mixed = jnp.dot(high[...], right[...], preferred_element_type=jnp.float32) + jnp.dot(
        low[...], right[...], preferred_element_type=jnp.float32
    )
    top = mixed.astype(jnp.bfloat16)
    high[...] = top
    low[...] = (mixed - top.astype(jnp.float32)).astype(jnp.bfloat16)
    for step in range(count):
        left = envs[step][0]
        part = jnp.dot(left, high[...], preferred_element_type=jnp.float32) + jnp.dot(
            left, low[...], preferred_element_type=jnp.float32
        )
        for half in range(HALVES):
            piece, out = part[:, half * width : (half + 1) * width], outs[half * count + step]
            if step == 0:
                out[...] = piece
            else:
                encode(piece, out, False)


def combine_kernel(base, sec, me, count, target_ref, *rest):
    parts, keep, send = rest[:count], rest[count], rest[count + 1]
    start, mine = base(), me()
    chip, core = sec() // 2, lax.rem(sec(), 2)
    keep[...] = jnp.zeros(keep.shape, jnp.float32)
    send[...] = jnp.zeros(send.shape, jnp.float32)
    for step in range(count):
        target = target_ref[start + mine ^ step]
        hop = (target // 2) ^ chip
        part = parts[0][...] if step == 0 else decode(parts[step])
        mine_too = lax.rem(target, 2) == core

        @pl.when(mine_too)
        def _():
            keep[hop] = keep[hop] + part

        @pl.when(jnp.logical_not(mine_too))
        def _():
            send[hop] = send[hop] + part


def join_kernel(chips, keep, other, *outs):
    for hop in range(chips):
        total = keep[hop] + other[hop]
        if hop == 0:
            outs[0][...] = total
        else:
            encode(total, outs[hop], False)


def finish_kernel(chips, *refs):
    width = refs[0].shape[1]
    for half in range(HALVES):
        mine = refs[half * chips : (half + 1) * chips]
        total = mine[0][...]
        for hop in range(1, chips):
            total = total + decode(mine[hop])
        refs[-1][:, half * width : (half + 1) * width] = total


def body(wavefunction, left_env, right_env, task_in, task_out, task_term):
    groups, count = lax.axis_size("sec"), lax.axis_size("env")
    chips = groups // 2
    _, rows, cols = wavefunction.shape
    per_device = task_in.shape[0] // (groups * count)
    targets = task_out[:, 0]
    f32, bf16 = jnp.float32, jnp.bfloat16
    block = jax.ShapeDtypeStruct((rows, cols), f32)
    sec = lambda: lax.axis_index("sec")
    me = lambda: lax.axis_index("env")

    def along(shift):
        return [(i, i ^ shift) for i in range(count)]

    def across(hop):
        return [(i, i ^ (2 * hop)) for i in range(groups)]

    def exchange(blocks):
        got = list(blocks)
        for s in far_first(count):
            got[s] = lax.ppermute(blocks[s], "env", along(s))
        return got

    pair = [(i, i ^ 1) for i in range(groups)]
    code = jax.ShapeDtypeStruct((rows + HEAD, cols), jnp.int16)
    width = cols // HALVES
    part = jax.ShapeDtypeStruct((rows, width), f32)
    piece = jax.ShapeDtypeStruct((rows + HEAD, width), jnp.int16)
    stack = jax.ShapeDtypeStruct((chips, rows, width), f32)

    keeps, sends, held = [None] * HALVES, [None] * HALVES, None
    for turn in range(per_device):
        base = lambda: (sec() * per_device + turn) * count
        partner_base = lambda: ((sec() ^ 1) * per_device + turn) * count
        env_block = jax.ShapeDtypeStruct((2, rows, cols), bf16)
        envs = call(
            functools.partial(pick_kernel, base, me, count),
            [env_block] * count,
            [SMEM, HBM, HBM],
            [pltpu.SemaphoreType.DMA((2 * count,))],
            vmem=PICK_BYTES,
        )(task_term, left_env, right_env)
        envs = exchange(envs)
        if held is None:
            psi = call(encode_kernel, code, [VMEM])(wavefunction[0])
            held = [psi] + [lax.ppermute(psi, "sec", across(hop)) for hop in range(1, chips)]
        sent = call(
            functools.partial(partner_psi_kernel, partner_base, sec, count, chips),
            jax.ShapeDtypeStruct((count, *code.shape), code.dtype),
            [SMEM] + [VMEM] * chips,
        )(task_in, *held)
        paired = lax.ppermute(sent, "sec", pair)
        psis = call(
            functools.partial(own_psi_kernel, base, sec, me, count, chips),
            [code] * count,
            [SMEM] + [VMEM] * (chips + 1),
        )(task_in, *held, paired)
        psis = exchange(psis)
        full = count * rows
        parts = call(
            functools.partial(task_kernel, me, count),
            ([part] + [piece] * (count - 1)) * HALVES,
            [VMEM] * (2 * count),
            [pltpu.VMEM((full, cols), bf16)] * 3,
            flops=8 * full * full * cols,
        )(*envs, *psis)
        halves = [parts[half * count : (half + 1) * count] for half in range(HALVES)]
        halves = [exchange(mine) for mine in halves]
        for half, mine in enumerate(halves):
            kept, sent = call(
                functools.partial(combine_kernel, base, sec, me, count),
                [stack, stack],
                [SMEM] + [VMEM] * count,
            )(targets, *mine)
            if turn:
                kept, sent = keeps[half] + kept, sends[half] + sent
            keeps[half], sends[half] = kept, sent
    sums = []
    for half in range(HALVES):
        other = lax.ppermute(sends[half], "sec", pair)
        mine = call(
            functools.partial(join_kernel, chips), [part] + [piece] * (chips - 1), [VMEM] * 2
        )(keeps[half], other)
        sums += [mine[0]]
        sums += [lax.ppermute(mine[hop], "sec", across(hop)) for hop in range(1, chips)]
    total = call(functools.partial(finish_kernel, chips), block, [VMEM] * (chips * HALVES))(*sums)
    return total[None]


def far_first(count):
    return sorted(range(1, count), key=lambda step: -step.bit_length())


def solution(mesh):
    placed = (P("sec", "env", None), P(None, "env", None), P(None, "env", None), P(), P(), P())
    return jax.shard_map(
        body, mesh=mesh, in_specs=placed, out_specs=P("sec", "env", None), check_vma=False
    )
```

```python
import functools

import jax
import jax.numpy as jnp
from jax import lax
from jax.experimental import pallas as pl
from jax.experimental.pallas import tpu as pltpu
from jax.sharding import PartitionSpec as P


GRID, LIMIT, LEVELS, HEAD, HALVES = 1024.0, 32767.0, 256.0, 8, 2
PICK_BYTES = 54_000_000
VMEM_BYTES = 16 * 1024 * 1024
VMEM = pl.BlockSpec(memory_space=pltpu.VMEM)
SMEM = pl.BlockSpec(memory_space=pltpu.SMEM)
HBM = pl.BlockSpec(memory_space=pltpu.HBM)


def call(kernel, out_shape, in_specs, scratch=(), flops=1, vmem=VMEM_BYTES):
    return pl.pallas_call(
        kernel,
        out_shape=out_shape,
        in_specs=in_specs,
        out_specs=jax.tree.map(lambda _: VMEM, out_shape),
        scratch_shapes=list(scratch),
        cost_estimate=pl.CostEstimate(flops=flops, bytes_accessed=1, transcendentals=0),
        compiler_params=pltpu.CompilerParams(vmem_limit_bytes=vmem),
    )


def encode(value, out, centred):
    rows = value.shape[0]
    centre = jnp.zeros_like(value[:1])
    if centred:
        middle = (jnp.max(value, axis=0, keepdims=True) + jnp.min(value, axis=0, keepdims=True)) / 2
        centre = jnp.clip((middle * GRID).astype(jnp.int32), -LIMIT, LIMIT).astype(jnp.float32)
        value = value - centre / GRID
    span = jnp.max(jnp.abs(value), axis=0, keepdims=True)
    level = jnp.log(jnp.maximum(span, 1e-30)) * LEVELS + 1.0
    level = (level + jnp.where(level > 0, 1.0, 0.0)).astype(jnp.int32).astype(jnp.float32)
    scaled = value * (LIMIT / jnp.exp(level / LEVELS))
    scaled = jnp.clip(scaled + jnp.where(scaled > 0, 0.5, -0.5), -LIMIT, LIMIT)
    out[pl.ds(0, rows), :] = scaled.astype(jnp.int32).astype(jnp.int16)
    lines = lax.broadcasted_iota(jnp.int32, (HEAD, value.shape[1]), 0)
    head = jnp.where(lines == 0, level.astype(jnp.int32), centre.astype(jnp.int32))
    out[pl.ds(rows, HEAD), :] = head.astype(jnp.int16)


def decode(code):
    rows = code.shape[0] - HEAD
    head = code[pl.ds(rows, HEAD), :].astype(jnp.int32).astype(jnp.float32)
    step = jnp.exp(head[0:1] / LEVELS) / LIMIT
    value = code[pl.ds(0, rows), :].astype(jnp.int32).astype(jnp.float32)
    return value * step + head[1:2] / GRID


def pick_kernel(base, me, count, term_ref, left_ref, right_ref, *rest):
    outs, sem = rest[:-1], rest[-1]
    _, cols = left_ref.shape[1:]
    width = cols // HALVES
    copies = []
    start, mine = base(), me()
    for step in range(count):
        term = term_ref[start + (mine ^ step)]
        copies.append((left_ref.at[term], outs[step].at[:, pl.ds(0, cols)]))
        for half in range(HALVES):
            out = outs[half * count + step]
            copies.append(
                (
                    right_ref.at[term, :, pl.ds(half * width, width)],
                    out if half else out.at[:, pl.ds(cols, width)],
                )
            )
    copies = [pltpu.make_async_copy(*copy, sem.at[i]) for i, copy in enumerate(copies)]
    for copy in copies:
        copy.start()
    for copy in copies:
        copy.wait()


def encode_kernel(psi_ref, code):
    encode(psi_ref[...], code, True)


def partner_psi_kernel(base, sec, count, chips, in_ref, *rest):
    held, out = rest[:chips], rest[chips]
    start = base()
    chip, core = sec() // 2, lax.rem(sec(), 2)
    for slot in range(count):
        source = in_ref[start + slot]
        for step in range(chips):
            @pl.when((source // 2 == chip ^ step) & (lax.rem(source, 2) == core))
            def _():
                out[slot] = held[step][...]


def own_psi_kernel(base, sec, me, count, chips, in_ref, *rest):
    held, paired, outs = rest[:chips], rest[chips], rest[chips + 1 :]
    start, mine = base(), me()
    chip, core = sec() // 2, lax.rem(sec(), 2)
    for step in range(count):
        slot = mine ^ step
        source = in_ref[start + slot]
        same = lax.rem(source, 2) == core
        for hop in range(chips):
            @pl.when((source // 2 == chip ^ hop) & same)
            def _():
                outs[step][...] = held[hop][...]

        @pl.when(jnp.logical_not(same))
        def _():
            outs[step][...] = paired[slot]


def task_kernel(me, count, half, *refs):
    envs, psis, lates, outs = refs[:count], refs[count : 2 * count], refs[2 * count : -3 - count], refs[-3 - count : -3]
    high, low, right = refs[-3:]
    rows, width = outs[0].shape
    cols = high.shape[1]
    mine = me()
    for step in range(count):
        place = pl.ds(pl.multiple_of((mine ^ step) * rows, rows), rows)
        right[place, :] = lates[step][...] if half else envs[step][:, pl.ds(cols, width)]
        psi = decode(psis[step])
        top = psi.astype(jnp.bfloat16)
        high[place, :] = top
        low[place, :] = (psi - top.astype(jnp.float32)).astype(jnp.bfloat16)
    mixed = jnp.dot(high[...], right[...], preferred_element_type=jnp.float32) + jnp.dot(
        low[...], right[...], preferred_element_type=jnp.float32
    )
    top = mixed.astype(jnp.bfloat16)
    rest = (mixed - top.astype(jnp.float32)).astype(jnp.bfloat16)
    for step in far_first(count) + [0]:
        left = envs[step][:, pl.ds(0, cols)]
        part = jnp.dot(left, top, preferred_element_type=jnp.float32) + jnp.dot(
            left, rest, preferred_element_type=jnp.float32
        )
        if step == 0:
            outs[step][...] = part
        else:
            encode(part, outs[step], False)


def combine_kernel(base, sec, me, count, target_ref, *rest):
    parts, keep, send = rest[:count], rest[count], rest[count + 1]
    start, mine = base(), me()
    chip, core = sec() // 2, lax.rem(sec(), 2)
    keep[...] = jnp.zeros(keep.shape, jnp.float32)
    send[...] = jnp.zeros(send.shape, jnp.float32)
    for step in range(count):
        target = target_ref[start + mine ^ step]
        hop = (target // 2) ^ chip
        part = parts[0][...] if step == 0 else decode(parts[step])
        mine_too = lax.rem(target, 2) == core

        @pl.when(mine_too)
        def _():
            keep[hop] = keep[hop] + part

        @pl.when(jnp.logical_not(mine_too))
        def _():
            send[hop] = send[hop] + part


def join_kernel(chips, keep, other, *outs):
    for hop in range(chips):
        total = keep[hop] + other[hop]
        if hop == 0:
            outs[0][...] = total
        else:
            encode(total, outs[hop], False)


def finish_kernel(chips, *refs):
    width = refs[0].shape[1]
    for half in range(HALVES):
        mine = refs[half * chips : (half + 1) * chips]
        total = mine[0][...]
        for hop in range(1, chips):
            total = total + decode(mine[hop])
        refs[-1][:, half * width : (half + 1) * width] = total


def body(wavefunction, left_env, right_env, task_in, task_out, task_term):
    groups, count = lax.axis_size("sec"), lax.axis_size("env")
    chips = groups // 2
    _, rows, cols = wavefunction.shape
    per_device = task_in.shape[0] // (groups * count)
    targets = task_out[:, 0]
    f32, bf16 = jnp.float32, jnp.bfloat16
    block = jax.ShapeDtypeStruct((rows, cols), f32)
    sec = lambda: lax.axis_index("sec")
    me = lambda: lax.axis_index("env")

    def along(shift):
        return [(i, i ^ shift) for i in range(count)]

    def across(hop):
        return [(i, i ^ (2 * hop)) for i in range(groups)]

    def exchange(blocks):
        got = list(blocks)
        for s in far_first(count):
            got[s] = lax.ppermute(blocks[s], "env", along(s))
        return got

    pair = [(i, i ^ 1) for i in range(groups)]
    code = jax.ShapeDtypeStruct((rows + HEAD, cols), jnp.int16)
    width = cols // HALVES
    part = jax.ShapeDtypeStruct((rows, width), f32)
    piece = jax.ShapeDtypeStruct((rows + HEAD, width), jnp.int16)
    stack = jax.ShapeDtypeStruct((chips, rows, width), f32)

    keeps, sends, held = [None] * HALVES, [None] * HALVES, None
    for turn in range(per_device):
        base = lambda: (sec() * per_device + turn) * count
        partner_base = lambda: ((sec() ^ 1) * per_device + turn) * count
        early = jax.ShapeDtypeStruct((rows, cols + width), bf16)
        late = jax.ShapeDtypeStruct((rows, width), bf16)
        picked = call(
            functools.partial(pick_kernel, base, me, count),
            [early] * count + [late] * (count * (HALVES - 1)),
            [SMEM, HBM, HBM],
            [pltpu.SemaphoreType.DMA((count * (HALVES + 1),))],
            vmem=PICK_BYTES,
        )(task_term, left_env, right_env)
        envs = exchange(picked[:count])
        if held is None:
            psi = call(encode_kernel, code, [VMEM])(wavefunction[0])
            held = [psi] + [lax.ppermute(psi, "sec", across(hop)) for hop in range(1, chips)]
        sent = call(
            functools.partial(partner_psi_kernel, partner_base, sec, count, chips),
            jax.ShapeDtypeStruct((count, *code.shape), code.dtype),
            [SMEM] + [VMEM] * chips,
        )(task_in, *held)
        paired = lax.ppermute(sent, "sec", pair)
        psis = call(
            functools.partial(own_psi_kernel, base, sec, me, count, chips),
            [code] * count,
            [SMEM] + [VMEM] * (chips + 1),
        )(task_in, *held, paired)
        psis = exchange(psis)
        lates = [exchange(picked[half * count : (half + 1) * count]) for half in range(1, HALVES)]
        full = count * rows
        halves = []
        for half in range(HALVES):
            extra = lates[half - 1] if half else []
            parts = call(
                functools.partial(task_kernel, me, count, half),
                [part] + [piece] * (count - 1),
                [VMEM] * (2 * count + len(extra)),
                [pltpu.VMEM((full, cols), bf16)] * 2 + [pltpu.VMEM((full, width), bf16)],
                flops=8 * full * full * width,
            )(*envs, *psis, *extra)
            halves.append(exchange(parts))
        for half, mine in enumerate(halves):
            kept, sent = call(
                functools.partial(combine_kernel, base, sec, me, count),
                [stack, stack],
                [SMEM] + [VMEM] * count,
            )(targets, *mine)
            if turn:
                kept, sent = keeps[half] + kept, sends[half] + sent
            keeps[half], sends[half] = kept, sent
    sums = []
    for half in range(HALVES):
        other = lax.ppermute(sends[half], "sec", pair)
        mine = call(
            functools.partial(join_kernel, chips), [part] + [piece] * (chips - 1), [VMEM] * 2
        )(keeps[half], other)
        sums += [mine[0]]
        sums += [lax.ppermute(mine[hop], "sec", across(hop)) for hop in range(1, chips)]
    total = call(functools.partial(finish_kernel, chips), block, [VMEM] * (chips * HALVES))(*sums)
    return total[None]


def far_first(count):
    return sorted(range(1, count), key=lambda step: -step.bit_length())


def solution(mesh):
    placed = (P("sec", "env", None), P(None, "env", None), P(None, "env", None), P(), P(), P())
    return jax.shard_map(
        body, mesh=mesh, in_specs=placed, out_specs=P("sec", "env", None), check_vma=False
    )
```

```python
import functools

import jax
import jax.numpy as jnp
from jax import lax
from jax.experimental import pallas as pl
from jax.experimental.pallas import tpu as pltpu
from jax.sharding import PartitionSpec as P


GRID, LIMIT, LEVELS, HEAD, HALVES = 1024.0, 32767.0, 256.0, 8, 2
PICK_BYTES = 54_000_000
VMEM_BYTES = 16 * 1024 * 1024
VMEM = pl.BlockSpec(memory_space=pltpu.VMEM)
SMEM = pl.BlockSpec(memory_space=pltpu.SMEM)
HBM = pl.BlockSpec(memory_space=pltpu.HBM)


def call(kernel, out_shape, in_specs, scratch=(), flops=1, vmem=VMEM_BYTES):
    return pl.pallas_call(
        kernel,
        out_shape=out_shape,
        in_specs=in_specs,
        out_specs=jax.tree.map(lambda _: VMEM, out_shape),
        scratch_shapes=list(scratch),
        cost_estimate=pl.CostEstimate(flops=flops, bytes_accessed=1, transcendentals=0),
        compiler_params=pltpu.CompilerParams(vmem_limit_bytes=vmem),
    )


def entry(table, index):
    places = lax.broadcasted_iota(jnp.int32, table.shape, 1)
    return jnp.sum(jnp.where(places == index, table[...], 0).astype(jnp.float32)).astype(jnp.int32)


def encode(value, out, centred):
    rows = value.shape[0]
    centre = jnp.zeros_like(value[:1])
    if centred:
        middle = (jnp.max(value, axis=0, keepdims=True) + jnp.min(value, axis=0, keepdims=True)) / 2
        centre = jnp.clip((middle * GRID).astype(jnp.int32), -LIMIT, LIMIT).astype(jnp.float32)
        value = value - centre / GRID
    span = jnp.max(jnp.abs(value), axis=0, keepdims=True)
    level = jnp.log(jnp.maximum(span, 1e-30)) * LEVELS + 1.0
    level = (level + jnp.where(level > 0, 1.0, 0.0)).astype(jnp.int32).astype(jnp.float32)
    scaled = value * (LIMIT / jnp.exp(level / LEVELS))
    scaled = jnp.clip(scaled + jnp.where(scaled > 0, 0.5, -0.5), -LIMIT, LIMIT)
    out[pl.ds(0, rows), :] = scaled.astype(jnp.int32).astype(jnp.int16)
    lines = lax.broadcasted_iota(jnp.int32, (HEAD, value.shape[1]), 0)
    head = jnp.where(lines == 0, level.astype(jnp.int32), centre.astype(jnp.int32))
    out[pl.ds(rows, HEAD), :] = head.astype(jnp.int16)


def decode(code):
    rows = code.shape[0] - HEAD
    head = code[pl.ds(rows, HEAD), :].astype(jnp.int32).astype(jnp.float32)
    step = jnp.exp(head[0:1] / LEVELS) / LIMIT
    value = code[pl.ds(0, rows), :].astype(jnp.int32).astype(jnp.float32)
    return value * step + head[1:2] / GRID


def pick_kernel(base, me, count, term_ref, left_ref, right_ref, *rest):
    outs, sem = rest[:-1], rest[-1]
    _, cols = left_ref.shape[1:]
    width = cols // HALVES
    copies = []
    start, mine = base(), me()
    for step in range(count):
        term = entry(term_ref, start + (mine ^ step))
        copies.append((left_ref.at[term], outs[step].at[:, pl.ds(0, cols)]))
        for half in range(HALVES):
            out = outs[half * count + step]
            copies.append(
                (
                    right_ref.at[term, :, pl.ds(half * width, width)],
                    out if half else out.at[:, pl.ds(cols, width)],
                )
            )
    copies = [pltpu.make_async_copy(*copy, sem.at[i]) for i, copy in enumerate(copies)]
    for copy in copies:
        copy.start()
    for copy in copies:
        copy.wait()


def encode_kernel(psi_ref, code):
    encode(psi_ref[...], code, True)


def partner_psi_kernel(base, sec, count, chips, in_ref, *rest):
    held, out = rest[:chips], rest[chips]
    start = base()
    chip, core = sec() // 2, lax.rem(sec(), 2)
    for slot in range(count):
        source = in_ref[start + slot]
        for step in range(chips):
            @pl.when((source // 2 == chip ^ step) & (lax.rem(source, 2) == core))
            def _():
                out[slot] = held[step][...]


def own_psi_kernel(base, sec, me, count, chips, in_ref, *rest):
    held, paired, outs = rest[:chips], rest[chips], rest[chips + 1 :]
    start, mine = base(), me()
    chip, core = sec() // 2, lax.rem(sec(), 2)
    for step in range(count):
        slot = mine ^ step
        source = in_ref[start + slot]
        same = lax.rem(source, 2) == core
        for hop in range(chips):
            @pl.when((source // 2 == chip ^ hop) & same)
            def _():
                outs[step][...] = held[hop][...]

        @pl.when(jnp.logical_not(same))
        def _():
            outs[step][...] = paired[slot]


def task_kernel(me, count, half, *refs):
    envs, psis, lates, outs = refs[:count], refs[count : 2 * count], refs[2 * count : -3 - count], refs[-3 - count : -3]
    high, low, right = refs[-3:]
    rows, width = outs[0].shape
    cols = high.shape[1]
    mine = me()
    for step in range(count):
        place = pl.ds(pl.multiple_of((mine ^ step) * rows, rows), rows)
        right[place, :] = lates[step][...] if half else envs[step][:, pl.ds(cols, width)]
        psi = decode(psis[step])
        top = psi.astype(jnp.bfloat16)
        high[place, :] = top
        low[place, :] = (psi - top.astype(jnp.float32)).astype(jnp.bfloat16)
    mixed = jnp.dot(high[...], right[...], preferred_element_type=jnp.float32) + jnp.dot(
        low[...], right[...], preferred_element_type=jnp.float32
    )
    top = mixed.astype(jnp.bfloat16)
    rest = (mixed - top.astype(jnp.float32)).astype(jnp.bfloat16)
    for step in far_first(count) + [0]:
        left = envs[step][:, pl.ds(0, cols)]
        part = jnp.dot(left, top, preferred_element_type=jnp.float32) + jnp.dot(
            left, rest, preferred_element_type=jnp.float32
        )
        if step == 0:
            outs[step][...] = part
        else:
            encode(part, outs[step], False)


def combine_kernel(base, sec, me, count, target_ref, *rest):
    parts, keep, send = rest[:count], rest[count], rest[count + 1]
    start, mine = base(), me()
    chip, core = sec() // 2, lax.rem(sec(), 2)
    keep[...] = jnp.zeros(keep.shape, jnp.float32)
    send[...] = jnp.zeros(send.shape, jnp.float32)
    for step in range(count):
        target = entry(target_ref, start + (mine ^ step))
        hop = (target // 2) ^ chip
        part = parts[0][...] if step == 0 else decode(parts[step])
        mine_too = lax.rem(target, 2) == core

        @pl.when(mine_too)
        def _():
            keep[hop] = keep[hop] + part

        @pl.when(jnp.logical_not(mine_too))
        def _():
            send[hop] = send[hop] + part


def join_kernel(chips, keep, other, *outs):
    for hop in range(chips):
        total = keep[hop] + other[hop]
        if hop == 0:
            outs[0][...] = total
        else:
            encode(total, outs[hop], False)


def finish_kernel(chips, *refs):
    width = refs[0].shape[1]
    for half in range(HALVES):
        mine = refs[half * chips : (half + 1) * chips]
        total = mine[0][...]
        for hop in range(1, chips):
            total = total + decode(mine[hop])
        refs[-1][:, half * width : (half + 1) * width] = total


def body(wavefunction, left_env, right_env, task_in, task_out, task_term):
    groups, count = lax.axis_size("sec"), lax.axis_size("env")
    chips = groups // 2
    _, rows, cols = wavefunction.shape
    per_device = task_in.shape[0] // (groups * count)
    targets = task_out[:, 0][None]
    f32, bf16 = jnp.float32, jnp.bfloat16
    block = jax.ShapeDtypeStruct((rows, cols), f32)
    sec = lambda: lax.axis_index("sec")
    me = lambda: lax.axis_index("env")

    def along(shift):
        return [(i, i ^ shift) for i in range(count)]

    def across(hop):
        return [(i, i ^ (2 * hop)) for i in range(groups)]

    def exchange(blocks):
        got = list(blocks)
        for s in far_first(count):
            got[s] = lax.ppermute(blocks[s], "env", along(s))
        return got

    pair = [(i, i ^ 1) for i in range(groups)]
    code = jax.ShapeDtypeStruct((rows + HEAD, cols), jnp.int16)
    width = cols // HALVES
    part = jax.ShapeDtypeStruct((rows, width), f32)
    piece = jax.ShapeDtypeStruct((rows + HEAD, width), jnp.int16)
    stack = jax.ShapeDtypeStruct((chips, rows, width), f32)

    keeps, sends, held = [None] * HALVES, [None] * HALVES, None
    for turn in range(per_device):
        base = lambda: (sec() * per_device + turn) * count
        partner_base = lambda: ((sec() ^ 1) * per_device + turn) * count
        early = jax.ShapeDtypeStruct((rows, cols + width), bf16)
        late = jax.ShapeDtypeStruct((rows, width), bf16)
        picked = call(
            functools.partial(pick_kernel, base, me, count),
            [early] * count + [late] * (count * (HALVES - 1)),
            [VMEM, HBM, HBM],
            [pltpu.SemaphoreType.DMA((count * (HALVES + 1),))],
            vmem=PICK_BYTES,
        )(task_term[None], left_env, right_env)
        envs = exchange(picked[:count])
        if held is None:
            psi = call(encode_kernel, code, [VMEM])(wavefunction[0])
            held = [psi] + [lax.ppermute(psi, "sec", across(hop)) for hop in range(1, chips)]
        sent = call(
            functools.partial(partner_psi_kernel, partner_base, sec, count, chips),
            jax.ShapeDtypeStruct((count, *code.shape), code.dtype),
            [SMEM] + [VMEM] * chips,
        )(task_in, *held)
        paired = lax.ppermute(sent, "sec", pair)
        psis = call(
            functools.partial(own_psi_kernel, base, sec, me, count, chips),
            [code] * count,
            [SMEM] + [VMEM] * (chips + 1),
        )(task_in, *held, paired)
        psis = exchange(psis)
        lates = [exchange(picked[half * count : (half + 1) * count]) for half in range(1, HALVES)]
        full = count * rows
        halves = []
        for half in range(HALVES):
            extra = lates[half - 1] if half else []
            parts = call(
                functools.partial(task_kernel, me, count, half),
                [part] + [piece] * (count - 1),
                [VMEM] * (2 * count + len(extra)),
                [pltpu.VMEM((full, cols), bf16)] * 2 + [pltpu.VMEM((full, width), bf16)],
                flops=8 * full * full * width,
            )(*envs, *psis, *extra)
            halves.append(exchange(parts))
        for half, mine in enumerate(halves):
            kept, sent = call(
                functools.partial(combine_kernel, base, sec, me, count),
                [stack, stack],
                [VMEM] * (count + 1),
            )(targets, *mine)
            if turn:
                kept, sent = keeps[half] + kept, sends[half] + sent
            keeps[half], sends[half] = kept, sent
    sums = []
    for half in range(HALVES):
        other = lax.ppermute(sends[half], "sec", pair)
        mine = call(
            functools.partial(join_kernel, chips), [part] + [piece] * (chips - 1), [VMEM] * 2
        )(keeps[half], other)
        sums += [mine[0]]
        sums += [lax.ppermute(mine[hop], "sec", across(hop)) for hop in range(1, chips)]
    total = call(functools.partial(finish_kernel, chips), block, [VMEM] * (chips * HALVES))(*sums)
    return total[None]


def far_first(count):
    return sorted(range(1, count), key=lambda step: -step.bit_length())


def solution(mesh):
    placed = (P("sec", "env", None), P(None, "env", None), P(None, "env", None), P(), P(), P())
    return jax.shard_map(
        body, mesh=mesh, in_specs=placed, out_specs=P("sec", "env", None), check_vma=False
    )
```

```python
import functools

import jax
import jax.numpy as jnp
from jax import lax
from jax.experimental import pallas as pl
from jax.experimental.pallas import tpu as pltpu
from jax.sharding import PartitionSpec as P


GRID, LIMIT, LEVELS, LANES, HALVES = 1024.0, 32767.0, 256.0, 128, 2
PICK_BYTES = 54_000_000
VMEM_BYTES = 16 * 1024 * 1024
VMEM = pl.BlockSpec(memory_space=pltpu.VMEM)
SMEM = pl.BlockSpec(memory_space=pltpu.SMEM)
HBM = pl.BlockSpec(memory_space=pltpu.HBM)


def call(kernel, out_shape, in_specs, scratch=(), flops=1, vmem=VMEM_BYTES):
    return pl.pallas_call(
        kernel,
        out_shape=out_shape,
        in_specs=in_specs,
        out_specs=jax.tree.map(lambda _: VMEM, out_shape),
        scratch_shapes=list(scratch),
        cost_estimate=pl.CostEstimate(flops=flops, bytes_accessed=1, transcendentals=0),
        compiler_params=pltpu.CompilerParams(vmem_limit_bytes=vmem),
    )


def entry(table, index):
    places = lax.broadcasted_iota(jnp.int32, table.shape, 1)
    return jnp.sum(jnp.where(places == index, table[...], 0).astype(jnp.float32)).astype(jnp.int32)


def coded(rows, cols):
    runs = cols // LANES
    return (runs * rows + -(-2 * runs // 8) * 8, LANES)


def encode(value, out, centred):
    rows, cols = value.shape
    runs = cols // LANES
    centre = jnp.zeros_like(value[:1])
    if centred:
        middle = (jnp.max(value, axis=0, keepdims=True) + jnp.min(value, axis=0, keepdims=True)) / 2
        centre = jnp.clip((middle * GRID).astype(jnp.int32), -LIMIT, LIMIT).astype(jnp.float32)
        value = value - centre / GRID
    span = jnp.max(jnp.abs(value), axis=0, keepdims=True)
    level = jnp.log(jnp.maximum(span, 1e-30)) * LEVELS + 1.0
    level = (level + jnp.where(level > 0, 1.0, 0.0)).astype(jnp.int32).astype(jnp.float32)
    scaled = value * (LIMIT / jnp.exp(level / LEVELS))
    scaled = jnp.clip(scaled + jnp.where(scaled > 0, 0.5, -0.5), -LIMIT, LIMIT)
    scaled = scaled.astype(jnp.int32).astype(jnp.int16)
    height = out.shape[0] - runs * rows
    lines = lax.broadcasted_iota(jnp.int32, (height, LANES), 0)
    head = jnp.zeros((height, LANES), jnp.float32)
    for run in range(runs):
        place = slice(run * LANES, (run + 1) * LANES)
        out[pl.ds(run * rows, rows), :] = scaled[:, place]
        head = jnp.where(lines == run, level[:, place], head)
        head = jnp.where(lines == runs + run, centre[:, place], head)
    out[pl.ds(runs * rows, height), :] = head.astype(jnp.int32).astype(jnp.int16)


def decode(code, rows, cols):
    runs = cols // LANES
    head = code[pl.ds(runs * rows, code.shape[0] - runs * rows), :].astype(jnp.int32).astype(jnp.float32)
    pieces = []
    for run in range(runs):
        step = jnp.exp(head[run : run + 1] / LEVELS) / LIMIT
        value = code[pl.ds(run * rows, rows), :].astype(jnp.int32).astype(jnp.float32)
        pieces.append(value * step + head[runs + run : runs + run + 1] / GRID)
    return jnp.concatenate(pieces, axis=1)


def pick_kernel(base, me, count, term_ref, left_ref, right_ref, *rest):
    outs, sem = rest[:-1], rest[-1]
    _, cols = left_ref.shape[1:]
    width = cols // HALVES
    copies = []
    start, mine = base(), me()
    terms = [entry(term_ref, start + (mine ^ step)) for step in range(count)]
    for step, term in enumerate(terms):
        copies.append((left_ref.at[term], outs[step].at[:, pl.ds(0, cols)]))
        for half in range(HALVES):
            out = outs[half * count + step]
            copies.append(
                (
                    right_ref.at[term, :, pl.ds(half * width, width)],
                    out if half else out.at[:, pl.ds(cols, width)],
                )
            )
    copies = [pltpu.make_async_copy(*copy, sem.at[i]) for i, copy in enumerate(copies)]
    for copy in copies:
        copy.start()
    for copy in copies:
        copy.wait()


def encode_kernel(psi_ref, code):
    encode(psi_ref[...], code, True)


def partner_psi_kernel(base, sec, count, chips, in_ref, *rest):
    held, out = rest[:chips], rest[chips]
    start = base()
    chip, core = sec() // 2, lax.rem(sec(), 2)
    sources = [entry(in_ref, start + slot) for slot in range(count)]
    for slot, source in enumerate(sources):
        for step in range(chips):
            @pl.when((source // 2 == chip ^ step) & (lax.rem(source, 2) == core))
            def _():
                out[slot] = held[step][...]


def own_psi_kernel(base, sec, me, count, chips, in_ref, *rest):
    held, paired, outs = rest[:chips], rest[chips], rest[chips + 1 :]
    start, mine = base(), me()
    chip, core = sec() // 2, lax.rem(sec(), 2)
    slots = [mine ^ step for step in range(count)]
    sources = [entry(in_ref, start + slot) for slot in slots]
    for step, (slot, source) in enumerate(zip(slots, sources)):
        same = lax.rem(source, 2) == core
        for hop in range(chips):
            @pl.when((source // 2 == chip ^ hop) & same)
            def _():
                outs[step][...] = held[hop][...]

        @pl.when(jnp.logical_not(same))
        def _():
            outs[step][...] = paired[slot]


def task_kernel(me, count, half, *refs):
    envs, psis, lates, outs = refs[:count], refs[count : 2 * count], refs[2 * count : -3 - count], refs[-3 - count : -3]
    high, low, right = refs[-3:]
    rows, width = outs[0].shape
    cols = high.shape[1]
    mine = me()
    for step in range(count):
        place = pl.ds(pl.multiple_of((mine ^ step) * rows, rows), rows)
        right[place, :] = lates[step][...] if half else envs[step][:, pl.ds(cols, width)]
        psi = decode(psis[step], rows, cols)
        top = psi.astype(jnp.bfloat16)
        high[place, :] = top
        low[place, :] = (psi - top.astype(jnp.float32)).astype(jnp.bfloat16)
    mixed = jnp.dot(high[...], right[...], preferred_element_type=jnp.float32) + jnp.dot(
        low[...], right[...], preferred_element_type=jnp.float32
    )
    top = mixed.astype(jnp.bfloat16)
    rest = (mixed - top.astype(jnp.float32)).astype(jnp.bfloat16)
    for step in far_first(count) + [0]:
        left = envs[step][:, pl.ds(0, cols)]
        part = jnp.dot(left, top, preferred_element_type=jnp.float32) + jnp.dot(
            left, rest, preferred_element_type=jnp.float32
        )
        if step == 0:
            outs[step][...] = part
        else:
            encode(part, outs[step], False)


def combine_kernel(base, sec, me, count, target_ref, *rest):
    parts, keep, send = rest[:count], rest[count], rest[count + 1]
    start, mine = base(), me()
    chip, core = sec() // 2, lax.rem(sec(), 2)
    keep[...] = jnp.zeros(keep.shape, jnp.float32)
    send[...] = jnp.zeros(send.shape, jnp.float32)
    targets = [entry(target_ref, start + (mine ^ step)) for step in range(count)]
    for step, target in enumerate(targets):
        hop = (target // 2) ^ chip
        part = parts[0][...] if step == 0 else decode(parts[step], *parts[0].shape)
        mine_too = lax.rem(target, 2) == core

        @pl.when(mine_too)
        def _():
            keep[hop] = keep[hop] + part

        @pl.when(jnp.logical_not(mine_too))
        def _():
            send[hop] = send[hop] + part


def join_kernel(chips, keep, other, *outs):
    for hop in range(chips):
        total = keep[hop] + other[hop]
        if hop == 0:
            outs[0][...] = total
        else:
            encode(total, outs[hop], False)


def finish_kernel(chips, *refs):
    width = refs[0].shape[1]
    for half in range(HALVES):
        mine = refs[half * chips : (half + 1) * chips]
        total = mine[0][...]
        for hop in range(1, chips):
            total = total + decode(mine[hop], *mine[0].shape)
        refs[-1][:, half * width : (half + 1) * width] = total


def body(wavefunction, left_env, right_env, task_in, task_out, task_term):
    groups, count = lax.axis_size("sec"), lax.axis_size("env")
    chips = groups // 2
    _, rows, cols = wavefunction.shape
    per_device = task_in.shape[0] // (groups * count)
    targets = task_out[:, 0][None]
    f32, bf16 = jnp.float32, jnp.bfloat16
    block = jax.ShapeDtypeStruct((rows, cols), f32)
    sec = lambda: lax.axis_index("sec")
    me = lambda: lax.axis_index("env")

    def along(shift):
        return [(i, i ^ shift) for i in range(count)]

    def across(hop):
        return [(i, i ^ (2 * hop)) for i in range(groups)]

    def exchange(blocks):
        got = list(blocks)
        for s in far_first(count):
            got[s] = lax.ppermute(blocks[s], "env", along(s))
        return got

    pair = [(i, i ^ 1) for i in range(groups)]
    code = jax.ShapeDtypeStruct(coded(rows, cols), jnp.int16)
    width = cols // HALVES
    part = jax.ShapeDtypeStruct((rows, width), f32)
    piece = jax.ShapeDtypeStruct(coded(rows, width), jnp.int16)
    stack = jax.ShapeDtypeStruct((chips, rows, width), f32)

    keeps, sends, held = [None] * HALVES, [None] * HALVES, None
    for turn in range(per_device):
        base = lambda: (sec() * per_device + turn) * count
        partner_base = lambda: ((sec() ^ 1) * per_device + turn) * count
        early = jax.ShapeDtypeStruct((rows, cols + width), bf16)
        late = jax.ShapeDtypeStruct((rows, width), bf16)
        picked = call(
            functools.partial(pick_kernel, base, me, count),
            [early] * count + [late] * (count * (HALVES - 1)),
            [VMEM, HBM, HBM],
            [pltpu.SemaphoreType.DMA((count * (HALVES + 1),))],
            vmem=PICK_BYTES,
        )(task_term[None], left_env, right_env)
        envs = exchange(picked[:count])
        if held is None:
            psi = call(encode_kernel, code, [VMEM])(wavefunction[0])
            held = [psi] + [lax.ppermute(psi, "sec", across(hop)) for hop in range(1, chips)]
        sent = call(
            functools.partial(partner_psi_kernel, partner_base, sec, count, chips),
            jax.ShapeDtypeStruct((count, *code.shape), code.dtype),
            [VMEM] * (chips + 1),
        )(task_in[None], *held)
        paired = lax.ppermute(sent, "sec", pair)
        psis = call(
            functools.partial(own_psi_kernel, base, sec, me, count, chips),
            [code] * count,
            [VMEM] * (chips + 2),
        )(task_in[None], *held, paired)
        psis = exchange(psis)
        lates = [exchange(picked[half * count : (half + 1) * count]) for half in range(1, HALVES)]
        full = count * rows
        halves = []
        for half in range(HALVES):
            extra = lates[half - 1] if half else []
            parts = call(
                functools.partial(task_kernel, me, count, half),
                [part] + [piece] * (count - 1),
                [VMEM] * (2 * count + len(extra)),
                [pltpu.VMEM((full, cols), bf16)] * 2 + [pltpu.VMEM((full, width), bf16)],
                flops=8 * full * full * width,
            )(*envs, *psis, *extra)
            halves.append(exchange(parts))
        for half, mine in enumerate(halves):
            kept, sent = call(
                functools.partial(combine_kernel, base, sec, me, count),
                [stack, stack],
                [VMEM] * (count + 1),
            )(targets, *mine)
            if turn:
                kept, sent = keeps[half] + kept, sends[half] + sent
            keeps[half], sends[half] = kept, sent
    sums = []
    for half in range(HALVES):
        other = lax.ppermute(sends[half], "sec", pair)
        mine = call(
            functools.partial(join_kernel, chips), [part] + [piece] * (chips - 1), [VMEM] * 2
        )(keeps[half], other)
        sums += [mine[0]]
        sums += [lax.ppermute(mine[hop], "sec", across(hop)) for hop in range(1, chips)]
    total = call(functools.partial(finish_kernel, chips), block, [VMEM] * (chips * HALVES))(*sums)
    return total[None]


def far_first(count):
    return sorted(range(1, count), key=lambda step: -step.bit_length())


def solution(mesh):
    placed = (P("sec", "env", None), P(None, "env", None), P(None, "env", None), P(), P(), P())
    return jax.shard_map(
        body, mesh=mesh, in_specs=placed, out_specs=P("sec", "env", None), check_vma=False
    )
```

```python
import functools

import jax
import jax.numpy as jnp
from jax import lax
from jax.experimental import pallas as pl
from jax.experimental.pallas import tpu as pltpu
from jax.sharding import PartitionSpec as P


GRID, LIMIT, LEVELS, LANES, HALVES = 1024.0, 32767.0, 256.0, 128, 2
PICK_BYTES = 54_000_000
VMEM_BYTES = 16 * 1024 * 1024
VMEM = pl.BlockSpec(memory_space=pltpu.VMEM)
SMEM = pl.BlockSpec(memory_space=pltpu.SMEM)
HBM = pl.BlockSpec(memory_space=pltpu.HBM)


def call(kernel, out_shape, in_specs, scratch=(), flops=1, vmem=VMEM_BYTES):
    return pl.pallas_call(
        kernel,
        out_shape=out_shape,
        in_specs=in_specs,
        out_specs=jax.tree.map(lambda _: VMEM, out_shape),
        scratch_shapes=list(scratch),
        cost_estimate=pl.CostEstimate(flops=flops, bytes_accessed=1, transcendentals=0),
        compiler_params=pltpu.CompilerParams(vmem_limit_bytes=vmem),
    )


def entry(table, index):
    places = lax.broadcasted_iota(jnp.int32, table.shape, 1)
    return jnp.sum(jnp.where(places == index, table[...], 0).astype(jnp.float32)).astype(jnp.int32)


def coded(rows, cols):
    runs = cols // LANES
    return (runs * rows + -(-2 * runs // 8) * 8, LANES)


def encode(value, out, centred):
    rows, cols = value.shape
    runs = cols // LANES
    centre = jnp.zeros_like(value[:1])
    if centred:
        middle = (jnp.max(value, axis=0, keepdims=True) + jnp.min(value, axis=0, keepdims=True)) / 2
        centre = jnp.clip((middle * GRID).astype(jnp.int32), -LIMIT, LIMIT).astype(jnp.float32)
        value = value - centre / GRID
    span = jnp.max(jnp.abs(value), axis=0, keepdims=True)
    level = jnp.log(jnp.maximum(span, 1e-30)) * LEVELS + 1.0
    level = (level + jnp.where(level > 0, 1.0, 0.0)).astype(jnp.int32).astype(jnp.float32)
    scaled = value * (LIMIT / jnp.exp(level / LEVELS))
    scaled = jnp.clip(scaled + jnp.where(scaled > 0, 0.5, -0.5), -LIMIT, LIMIT)
    scaled = scaled.astype(jnp.int32).astype(jnp.int16)
    height = out.shape[0] - runs * rows
    lines = lax.broadcasted_iota(jnp.int32, (height, LANES), 0)
    head = jnp.zeros((height, LANES), jnp.float32)
    for run in range(runs):
        place = slice(run * LANES, (run + 1) * LANES)
        out[pl.ds(run * rows, rows), :] = scaled[:, place]
        head = jnp.where(lines == run, level[:, place], head)
        head = jnp.where(lines == runs + run, centre[:, place], head)
    out[pl.ds(runs * rows, height), :] = head.astype(jnp.int32).astype(jnp.int16)


def decode(code, rows, cols):
    runs = cols // LANES
    head = code[pl.ds(runs * rows, code.shape[0] - runs * rows), :].astype(jnp.int32).astype(jnp.float32)
    pieces = []
    for run in range(runs):
        step = jnp.exp(head[run : run + 1] / LEVELS) / LIMIT
        value = code[pl.ds(run * rows, rows), :].astype(jnp.int32).astype(jnp.float32)
        pieces.append(value * step + head[runs + run : runs + run + 1] / GRID)
    return jnp.concatenate(pieces, axis=1)


def pick_kernel(base, me, count, term_ref, left_ref, right_ref, *rest):
    outs, sem = rest[:-1], rest[-1]
    _, cols = left_ref.shape[1:]
    width = cols // HALVES
    copies = []
    start, mine = base(), me()
    terms = [entry(term_ref, start + (mine ^ step)) for step in range(count)]
    for step, term in enumerate(terms):
        copies.append((left_ref.at[term], outs[step].at[:, pl.ds(0, cols)]))
        for half in range(HALVES):
            out = outs[half * count + step]
            copies.append(
                (
                    right_ref.at[term, :, pl.ds(half * width, width)],
                    out if half else out.at[:, pl.ds(cols, width)],
                )
            )
    copies = [pltpu.make_async_copy(*copy, sem.at[i]) for i, copy in enumerate(copies)]
    for copy in copies:
        copy.start()
    for copy in copies:
        copy.wait()


def encode_kernel(psi_ref, code):
    encode(psi_ref[...], code, True)


def partner_psi_kernel(base, sec, me, count, chips, in_ref, *rest):
    held, out = rest[: 2 * chips], rest[2 * chips]
    start, mine, near = base(), me(), count // 2
    chip, core = sec() // 2, lax.rem(sec(), 2)
    sources = [entry(in_ref, start + (mine ^ step)) for step in range(near)]
    for step, source in enumerate(sources):
        for hop in range(chips):
            @pl.when((source // 2 == chip ^ hop) & (lax.rem(source, 2) == core))
            def _():
                out[step] = held[hop][...]
                out[near + step] = held[chips + hop][...]


def own_psi_kernel(base, sec, me, count, chips, in_ref, *rest):
    held, paired, outs = rest[: 2 * chips], rest[2 * chips], rest[2 * chips + 1 :]
    start, mine, near = base(), me(), count // 2
    chip, core = sec() // 2, lax.rem(sec(), 2)
    sources = [entry(in_ref, start + (mine ^ step)) for step in range(near)]
    for step, source in enumerate(sources):
        same = lax.rem(source, 2) == core
        for hop in range(chips):
            @pl.when((source // 2 == chip ^ hop) & same)
            def _():
                outs[step][0] = held[hop][...]
                outs[step][1] = held[chips + hop][...]

        @pl.when(jnp.logical_not(same))
        def _():
            outs[step][0] = paired[step]
            outs[step][1] = paired[near + step]


def task_kernel(me, count, half, *refs):
    near = count // 2
    envs, psis, lates, outs = (
        refs[:count],
        refs[count : count + near],
        refs[count + near : -3 - count],
        refs[-3 - count : -3],
    )
    psis = [both.at[0] for both in psis] + [both.at[1] for both in psis]
    high, low, right = refs[-3:]
    rows, width = outs[0].shape
    cols = high.shape[1]
    mine = me()
    for step in range(count):
        place = pl.ds(pl.multiple_of((mine ^ step) * rows, rows), rows)
        right[place, :] = lates[step][...] if half else envs[step][:, pl.ds(cols, width)]
        psi = decode(psis[step], rows, cols)
        top = psi.astype(jnp.bfloat16)
        high[place, :] = top
        low[place, :] = (psi - top.astype(jnp.float32)).astype(jnp.bfloat16)
    mixed = jnp.dot(high[...], right[...], preferred_element_type=jnp.float32) + jnp.dot(
        low[...], right[...], preferred_element_type=jnp.float32
    )
    top = mixed.astype(jnp.bfloat16)
    rest = (mixed - top.astype(jnp.float32)).astype(jnp.bfloat16)
    for step in far_first(count) + [0]:
        left = envs[step][:, pl.ds(0, cols)]
        part = jnp.dot(left, top, preferred_element_type=jnp.float32) + jnp.dot(
            left, rest, preferred_element_type=jnp.float32
        )
        if step == 0:
            outs[step][...] = part
        else:
            encode(part, outs[step], False)


def combine_kernel(base, sec, me, count, chips, target_ref, *rest):
    parts, (keep, code, send) = rest[:count], rest[count:]
    start, mine = base(), me()
    chip, core = sec() // 2, lax.rem(sec(), 2)
    keep[...] = jnp.zeros(keep.shape, jnp.float32)
    send[...] = jnp.zeros(send.shape, jnp.float32)
    targets = [entry(target_ref, start + (mine ^ step)) for step in range(count)]
    for step, target in enumerate(targets):
        hop = (target // 2) ^ chip
        part = parts[0][...] if step == 0 else decode(parts[step], *parts[0].shape)
        mine_too = lax.rem(target, 2) == core

        @pl.when(mine_too)
        def _():
            keep[hop] = keep[hop] + part

        @pl.when(jnp.logical_not(mine_too))
        def _():
            send[hop] = send[hop] + part

    for hop in range(chips):
        encode(send[hop], code.at[hop], False)


def join_kernel(chips, keep, other, *outs):
    for hop in range(chips):
        total = keep[hop] + decode(other.at[hop], *keep.shape[1:])
        if hop == 0:
            outs[0][...] = total
        else:
            encode(total, outs[hop], False)


def halve_kernel(first, second, keep, send):
    left = keep.shape[0]
    for slot in range(2 * left):
        if len(second.shape) == len(first.shape) and second.dtype == first.dtype:
            total = first[slot] + second[slot]
        else:
            total = first[slot] + decode(second.at[slot], *first.shape[1:])
        if slot < left:
            keep[slot] = total
        else:
            encode(total, send.at[slot - left], False)


def finish_kernel(counts, *refs):
    refs, out = list(refs[:-1]), refs[-1]
    place = 0
    for many in counts:
        mine, refs = refs[:many], refs[many:]
        rows, width = mine[0].shape[-2:]
        total = mine[0][...].reshape(rows, width)
        for code in mine[1:]:
            total = total + decode(code.at[0] if len(code.shape) > 2 else code, rows, width)
        out[:, place : place + width] = total
        place += width


def body(wavefunction, left_env, right_env, task_in, task_out, task_term):
    groups, count = lax.axis_size("sec"), lax.axis_size("env")
    chips = groups // 2
    _, rows, cols = wavefunction.shape
    per_device = task_in.shape[0] // (groups * count)
    targets = task_out[:, 0][None]
    f32, bf16 = jnp.float32, jnp.bfloat16
    block = jax.ShapeDtypeStruct((rows, cols), f32)
    sec = lambda: lax.axis_index("sec")
    me = lambda: lax.axis_index("env")

    def along(shift):
        return [(i, i ^ shift) for i in range(count)]

    def across(hop):
        return [(i, i ^ (2 * hop)) for i in range(groups)]

    def exchange(blocks):
        got = list(blocks)
        for s in far_first(count):
            got[s] = lax.ppermute(blocks[s], "env", along(s))
        return got

    pair = [(i, i ^ 1) for i in range(groups)]
    code = jax.ShapeDtypeStruct(coded(rows, cols), jnp.int16)
    width = cols // HALVES
    part = jax.ShapeDtypeStruct((rows, width), f32)
    piece = jax.ShapeDtypeStruct(coded(rows, width), jnp.int16)
    stack = jax.ShapeDtypeStruct((chips, rows, width), f32)

    keeps, sends, held = [None] * HALVES, [None] * HALVES, None
    for turn in range(per_device):
        base = lambda: (sec() * per_device + turn) * count
        partner_base = lambda: ((sec() ^ 1) * per_device + turn) * count
        early = jax.ShapeDtypeStruct((rows, cols + width), bf16)
        late = jax.ShapeDtypeStruct((rows, width), bf16)
        picked = call(
            functools.partial(pick_kernel, base, me, count),
            [early] * count + [late] * (count * (HALVES - 1)),
            [VMEM, HBM, HBM],
            [pltpu.SemaphoreType.DMA((count * (HALVES + 1),))],
            vmem=PICK_BYTES,
        )(task_term[None], left_env, right_env)
        envs = exchange(picked[:count])
        if held is None:
            psi = call(encode_kernel, code, [VMEM])(wavefunction[0])
            far = lax.ppermute(psi, "env", along(count // 2))
            held = []
            for rows_of in (psi, far):
                held += [rows_of] + [
                    lax.ppermute(rows_of, "sec", across(hop)) for hop in range(1, chips)
                ]
        sent = call(
            functools.partial(partner_psi_kernel, partner_base, sec, me, count, chips),
            jax.ShapeDtypeStruct((count, *code.shape), code.dtype),
            [VMEM] * (2 * chips + 1),
        )(task_in[None], *held)
        paired = lax.ppermute(sent, "sec", pair)
        psis = call(
            functools.partial(own_psi_kernel, base, sec, me, count, chips),
            [jax.ShapeDtypeStruct((2, *code.shape), code.dtype)] * (count // 2),
            [VMEM] * (2 * chips + 2),
        )(task_in[None], *held, paired)
        psis = [psis[0]] + [lax.ppermute(psis[s], "env", along(s)) for s in range(1, count // 2)]
        lates = [exchange(picked[half * count : (half + 1) * count]) for half in range(1, HALVES)]
        full = count * rows
        halves = []
        for half in range(HALVES):
            extra = lates[half - 1] if half else []
            parts = call(
                functools.partial(task_kernel, me, count, half),
                [part] + [piece] * (count - 1),
                [VMEM] * (count + count // 2 + len(extra)),
                [pltpu.VMEM((full, cols), bf16)] * 2 + [pltpu.VMEM((full, width), bf16)],
                flops=8 * full * full * width,
            )(*envs, *psis, *extra)
            halves.append(exchange(parts))
        for half, mine in enumerate(halves):
            kept, sent = call(
                functools.partial(combine_kernel, base, sec, me, count, chips),
                [stack, jax.ShapeDtypeStruct((chips, *piece.shape), piece.dtype)],
                [VMEM] * (count + 1),
                [pltpu.VMEM(stack.shape, f32)],
            )(targets, *mine)
            if turn:
                raise NotImplementedError
            keeps[half], sends[half] = kept, sent
    waves = []
    for half in range(HALVES):
        other = lax.ppermute(sends[half], "sec", pair)
        if half < HALVES - 1:
            bit, kept = chips // 2, keeps[half]
            while bit:
                kept, sent = call(
                    halve_kernel,
                    [
                        jax.ShapeDtypeStruct((bit, rows, width), f32),
                        jax.ShapeDtypeStruct((bit, *piece.shape), piece.dtype),
                    ],
                    [VMEM] * 2,
                )(kept, other)
                other = lax.ppermute(sent, "sec", across(bit))
                bit //= 2
            waves.append([kept, other])
            continue
        mine = call(
            functools.partial(join_kernel, chips), [part] + [piece] * (chips - 1), [VMEM] * 2
        )(keeps[half], other)
        waves.append(
            [mine[0]]
            + [lax.ppermute(mine[hop], "sec", across(hop)) for hop in range(1, chips)]
        )
    inputs = [value for wave in waves for value in wave]
    total = call(
        functools.partial(finish_kernel, [len(wave) for wave in waves]), block, [VMEM] * len(inputs)
    )(*inputs)
    return total[None]


def far_first(count):
    return sorted(range(1, count), key=lambda step: -step.bit_length())


def solution(mesh):
    placed = (P("sec", "env", None), P(None, "env", None), P(None, "env", None), P(), P(), P())
    return jax.shard_map(
        body, mesh=mesh, in_specs=placed, out_specs=P("sec", "env", None), check_vma=False
    )
```

```python
import functools

import jax
import jax.numpy as jnp
from jax import lax
from jax.experimental import pallas as pl
from jax.experimental.pallas import tpu as pltpu
from jax.sharding import PartitionSpec as P


GRID, LIMIT, LEVELS, LANES, HALVES = 1024.0, 32767.0, 256.0, 128, 2
PICK_BYTES = 54_000_000
VMEM_BYTES = 16 * 1024 * 1024
VMEM = pl.BlockSpec(memory_space=pltpu.VMEM)
SMEM = pl.BlockSpec(memory_space=pltpu.SMEM)
HBM = pl.BlockSpec(memory_space=pltpu.HBM)


def call(kernel, out_shape, in_specs, scratch=(), flops=1, vmem=VMEM_BYTES):
    return pl.pallas_call(
        kernel,
        out_shape=out_shape,
        in_specs=in_specs,
        out_specs=jax.tree.map(lambda _: VMEM, out_shape),
        scratch_shapes=list(scratch),
        cost_estimate=pl.CostEstimate(flops=flops, bytes_accessed=1, transcendentals=0),
        compiler_params=pltpu.CompilerParams(vmem_limit_bytes=vmem),
    )


def entry(table, index):
    places = lax.broadcasted_iota(jnp.int32, table.shape, 1)
    return jnp.sum(jnp.where(places == index, table[...], 0).astype(jnp.float32)).astype(jnp.int32)


def coded(rows, cols):
    runs = cols // LANES
    return (runs * rows + -(-2 * runs // 8) * 8, LANES)


def encode(value, out, centred):
    rows, cols = value.shape
    runs = cols // LANES
    centre = jnp.zeros_like(value[:1])
    if centred:
        middle = (jnp.max(value, axis=0, keepdims=True) + jnp.min(value, axis=0, keepdims=True)) / 2
        centre = jnp.clip((middle * GRID).astype(jnp.int32), -LIMIT, LIMIT).astype(jnp.float32)
        value = value - centre / GRID
    span = jnp.max(jnp.abs(value), axis=0, keepdims=True)
    level = jnp.log(jnp.maximum(span, 1e-30)) * LEVELS + 1.0
    level = (level + jnp.where(level > 0, 1.0, 0.0)).astype(jnp.int32).astype(jnp.float32)
    scaled = value * (LIMIT / jnp.exp(level / LEVELS))
    scaled = jnp.clip(scaled + jnp.where(scaled > 0, 0.5, -0.5), -LIMIT, LIMIT)
    scaled = scaled.astype(jnp.int32).astype(jnp.int16)
    height = out.shape[0] - runs * rows
    lines = lax.broadcasted_iota(jnp.int32, (height, LANES), 0)
    head = jnp.zeros((height, LANES), jnp.float32)
    for run in range(runs):
        place = slice(run * LANES, (run + 1) * LANES)
        out[pl.ds(run * rows, rows), :] = scaled[:, place]
        head = jnp.where(lines == run, level[:, place], head)
        head = jnp.where(lines == runs + run, centre[:, place], head)
    out[pl.ds(runs * rows, height), :] = head.astype(jnp.int32).astype(jnp.int16)


def decode(code, rows, cols):
    runs = cols // LANES
    head = code[pl.ds(runs * rows, code.shape[0] - runs * rows), :].astype(jnp.int32).astype(jnp.float32)
    pieces = []
    for run in range(runs):
        step = jnp.exp(head[run : run + 1] / LEVELS) / LIMIT
        value = code[pl.ds(run * rows, rows), :].astype(jnp.int32).astype(jnp.float32)
        pieces.append(value * step + head[runs + run : runs + run + 1] / GRID)
    return jnp.concatenate(pieces, axis=1)


def pick_kernel(base, me, count, term_ref, left_ref, right_ref, *rest):
    outs, sem = rest[:-1], rest[-1]
    _, cols = left_ref.shape[1:]
    width = cols // HALVES
    copies = []
    start, mine = base(), me()
    terms = [entry(term_ref, start + (mine ^ step)) for step in range(count)]
    for step, term in enumerate(terms):
        copies.append((left_ref.at[term], outs[step].at[:, pl.ds(0, cols)]))
        for half in range(HALVES):
            out = outs[half * count + step]
            copies.append(
                (
                    right_ref.at[term, :, pl.ds(half * width, width)],
                    out if half else out.at[:, pl.ds(cols, width)],
                )
            )
    copies = [pltpu.make_async_copy(*copy, sem.at[i]) for i, copy in enumerate(copies)]
    for copy in copies:
        copy.start()
    for copy in copies:
        copy.wait()


def encode_kernel(psi_ref, code):
    encode(psi_ref[...], code, True)


def partner_psi_kernel(base, sec, me, count, chips, in_ref, *rest):
    held, out = rest[: 2 * chips], rest[2 * chips]
    start, mine, near = base(), me(), count // 2
    chip, core = sec() // 2, lax.rem(sec(), 2)
    sources = [entry(in_ref, start + (mine ^ step)) for step in range(near)]
    for step, source in enumerate(sources):
        for hop in range(chips):
            @pl.when((source // 2 == chip ^ hop) & (lax.rem(source, 2) == core))
            def _():
                out[step] = held[hop][...]
                out[near + step] = held[chips + hop][...]


def own_psi_kernel(base, sec, me, count, chips, in_ref, *rest):
    held, paired, outs = rest[: 2 * chips], rest[2 * chips], rest[2 * chips + 1 :]
    start, mine, near = base(), me(), count // 2
    chip, core = sec() // 2, lax.rem(sec(), 2)
    sources = [entry(in_ref, start + (mine ^ step)) for step in range(near)]
    for step, source in enumerate(sources):
        same = lax.rem(source, 2) == core
        for hop in range(chips):
            @pl.when((source // 2 == chip ^ hop) & same)
            def _():
                outs[step][0] = held[hop][...]
                outs[step][1] = held[chips + hop][...]

        @pl.when(jnp.logical_not(same))
        def _():
            outs[step][0] = paired[step]
            outs[step][1] = paired[near + step]


def task_kernel(me, count, half, *refs):
    near = count // 2
    envs, psis, lates, outs = (
        refs[:count],
        refs[count : count + near],
        refs[count + near : -3 - count],
        refs[-3 - count : -3],
    )
    psis = [both.at[0] for both in psis] + [both.at[1] for both in psis]
    high, low, right = refs[-3:]
    rows, width = outs[0].shape
    cols = high.shape[1]
    mine = me()
    for step in range(count):
        place = pl.ds(pl.multiple_of((mine ^ step) * rows, rows), rows)
        right[place, :] = lates[step][...] if half else envs[step][:, pl.ds(cols, width)]
        psi = decode(psis[step], rows, cols)
        top = psi.astype(jnp.bfloat16)
        high[place, :] = top
        low[place, :] = (psi - top.astype(jnp.float32)).astype(jnp.bfloat16)
    mixed = jnp.dot(high[...], right[...], preferred_element_type=jnp.float32) + jnp.dot(
        low[...], right[...], preferred_element_type=jnp.float32
    )
    top = mixed.astype(jnp.bfloat16)
    rest = (mixed - top.astype(jnp.float32)).astype(jnp.bfloat16)
    for step in far_first(count) + [0]:
        left = envs[step][:, pl.ds(0, cols)]
        part = jnp.dot(left, top, preferred_element_type=jnp.float32) + jnp.dot(
            left, rest, preferred_element_type=jnp.float32
        )
        if step == 0:
            outs[step][...] = part
        else:
            encode(part, outs[step], False)


def combine_kernel(base, sec, me, count, target_ref, *rest):
    parts, keep, send = rest[:count], rest[count], rest[count + 1]
    start, mine = base(), me()
    chip, core = sec() // 2, lax.rem(sec(), 2)
    keep[...] = jnp.zeros(keep.shape, jnp.float32)
    send[...] = jnp.zeros(send.shape, jnp.float32)
    targets = [entry(target_ref, start + (mine ^ step)) for step in range(count)]
    for step, target in enumerate(targets):
        hop = (target // 2) ^ chip
        part = parts[0][...] if step == 0 else decode(parts[step], *parts[0].shape)
        mine_too = lax.rem(target, 2) == core

        @pl.when(mine_too)
        def _():
            keep[hop] = keep[hop] + part

        @pl.when(jnp.logical_not(mine_too))
        def _():
            send[hop] = send[hop] + part


def join_kernel(chips, keep, other, *outs):
    for hop in range(chips):
        total = keep[hop] + other[hop]
        if hop == 0:
            outs[0][...] = total
        else:
            encode(total, outs[hop], False)


def halve_kernel(first, second, keep, send):
    left = keep.shape[0]
    for slot in range(2 * left):
        if len(second.shape) == len(first.shape) and second.dtype == first.dtype:
            total = first[slot] + second[slot]
        else:
            total = first[slot] + decode(second.at[slot], *first.shape[1:])
        if slot < left:
            keep[slot] = total
        else:
            encode(total, send.at[slot - left], False)


def finish_kernel(counts, *refs):
    refs, out = list(refs[:-1]), refs[-1]
    place = 0
    for many in counts:
        mine, refs = refs[:many], refs[many:]
        rows, width = mine[0].shape[-2:]
        total = mine[0][...].reshape(rows, width)
        for code in mine[1:]:
            total = total + decode(code.at[0] if len(code.shape) > 2 else code, rows, width)
        out[:, place : place + width] = total
        place += width


def body(wavefunction, left_env, right_env, task_in, task_out, task_term):
    groups, count = lax.axis_size("sec"), lax.axis_size("env")
    chips = groups // 2
    _, rows, cols = wavefunction.shape
    per_device = task_in.shape[0] // (groups * count)
    targets = task_out[:, 0][None]
    f32, bf16 = jnp.float32, jnp.bfloat16
    block = jax.ShapeDtypeStruct((rows, cols), f32)
    sec = lambda: lax.axis_index("sec")
    me = lambda: lax.axis_index("env")

    def along(shift):
        return [(i, i ^ shift) for i in range(count)]

    def across(hop):
        return [(i, i ^ (2 * hop)) for i in range(groups)]

    def exchange(blocks):
        got = list(blocks)
        for s in far_first(count):
            got[s] = lax.ppermute(blocks[s], "env", along(s))
        return got

    pair = [(i, i ^ 1) for i in range(groups)]
    code = jax.ShapeDtypeStruct(coded(rows, cols), jnp.int16)
    width = cols // HALVES
    part = jax.ShapeDtypeStruct((rows, width), f32)
    piece = jax.ShapeDtypeStruct(coded(rows, width), jnp.int16)
    stack = jax.ShapeDtypeStruct((chips, rows, width), f32)

    keeps, sends, held = [None] * HALVES, [None] * HALVES, None
    for turn in range(per_device):
        base = lambda: (sec() * per_device + turn) * count
        partner_base = lambda: ((sec() ^ 1) * per_device + turn) * count
        early = jax.ShapeDtypeStruct((rows, cols + width), bf16)
        late = jax.ShapeDtypeStruct((rows, width), bf16)
        picked = call(
            functools.partial(pick_kernel, base, me, count),
            [early] * count + [late] * (count * (HALVES - 1)),
            [VMEM, HBM, HBM],
            [pltpu.SemaphoreType.DMA((count * (HALVES + 1),))],
            vmem=PICK_BYTES,
        )(task_term[None], left_env, right_env)
        envs = exchange(picked[:count])
        if held is None:
            psi = call(encode_kernel, code, [VMEM])(wavefunction[0])
            far = lax.ppermute(psi, "env", along(count // 2))
            held = []
            for rows_of in (psi, far):
                held += [rows_of] + [
                    lax.ppermute(rows_of, "sec", across(hop)) for hop in range(1, chips)
                ]
        sent = call(
            functools.partial(partner_psi_kernel, partner_base, sec, me, count, chips),
            jax.ShapeDtypeStruct((count, *code.shape), code.dtype),
            [VMEM] * (2 * chips + 1),
        )(task_in[None], *held)
        paired = lax.ppermute(sent, "sec", pair)
        psis = call(
            functools.partial(own_psi_kernel, base, sec, me, count, chips),
            [jax.ShapeDtypeStruct((2, *code.shape), code.dtype)] * (count // 2),
            [VMEM] * (2 * chips + 2),
        )(task_in[None], *held, paired)
        psis = [psis[0]] + [lax.ppermute(psis[s], "env", along(s)) for s in range(1, count // 2)]
        lates = [exchange(picked[half * count : (half + 1) * count]) for half in range(1, HALVES)]
        full = count * rows
        halves = []
        for half in range(HALVES):
            extra = lates[half - 1] if half else []
            parts = call(
                functools.partial(task_kernel, me, count, half),
                [part] + [piece] * (count - 1),
                [VMEM] * (count + count // 2 + len(extra)),
                [pltpu.VMEM((full, cols), bf16)] * 2 + [pltpu.VMEM((full, width), bf16)],
                flops=8 * full * full * width,
            )(*envs, *psis, *extra)
            halves.append(exchange(parts))
        for half, mine in enumerate(halves):
            kept, sent = call(
                functools.partial(combine_kernel, base, sec, me, count),
                [stack, stack],
                [VMEM] * (count + 1),
            )(targets, *mine)
            if turn:
                kept, sent = keeps[half] + kept, sends[half] + sent
            keeps[half], sends[half] = kept, sent
    waves = []
    for half in range(HALVES):
        other = lax.ppermute(sends[half], "sec", pair)
        if half < HALVES - 1:
            bit, kept = chips // 2, keeps[half]
            while bit:
                kept, sent = call(
                    halve_kernel,
                    [
                        jax.ShapeDtypeStruct((bit, rows, width), f32),
                        jax.ShapeDtypeStruct((bit, *piece.shape), piece.dtype),
                    ],
                    [VMEM] * 2,
                )(kept, other)
                other = lax.ppermute(sent, "sec", across(bit))
                bit //= 2
            waves.append([kept, other])
            continue
        mine = call(
            functools.partial(join_kernel, chips), [part] + [piece] * (chips - 1), [VMEM] * 2
        )(keeps[half], other)
        waves.append(
            [mine[0]]
            + [lax.ppermute(mine[hop], "sec", across(hop)) for hop in range(1, chips)]
        )
    inputs = [value for wave in waves for value in wave]
    total = call(
        functools.partial(finish_kernel, [len(wave) for wave in waves]), block, [VMEM] * len(inputs)
    )(*inputs)
    return total[None]


def far_first(count):
    return sorted(range(1, count), key=lambda step: -step.bit_length())


def solution(mesh):
    placed = (P("sec", "env", None), P(None, "env", None), P(None, "env", None), P(), P(), P())
    return jax.shard_map(
        body, mesh=mesh, in_specs=placed, out_specs=P("sec", "env", None), check_vma=False
    )
```
